32 devices in a mesh: comp: 2 (over core), tile: 16 (over z, y, x).
Axes of the slice: x: 2, y: 2, z: 4, core: 2. Of those that a mesh axis runs over, the one named last changes fastest.
Arguments:
- state: bfloat16 [2, 256, 4, 60, 128], P('comp', 'tile'), may hold values from -6 to 6
- dyn_weights: bfloat16 [2, 64, 128, 128], P('comp'), may hold values from -0.1875 to 0.1875
- vertical: float32 [2, 60, 60], P('comp'), may hold values from -0.75 to 0.75
- remap_weights: bfloat16 [2, 64, 128, 128], replicated, may hold values from -0.5 to 0.5
- neighbor_slots: int32 [2, 256, 4], P('comp', 'tile'), may hold values from 0 to 39
- neighbor_tiles: int32 [2, 256, 4], P('comp', 'tile'), may hold values from 0 to 63
- remap_source: int32 [2, 256], P('comp', 'tile'), may hold values from 0 to 15
- remap_target: int32 [2, 256], P('comp', 'tile'), may hold values from 0 to 15
- remap_tile: int32 [2, 256], P('comp', 'tile'), may hold values from 0 to 63
- remap_dest: int32 [2, 256, 1], P('comp', 'tile'), may hold values from 0 to 15, as said below
Outputs:
- new_state: bfloat16 [2, 256, 4, 60, 128], P('comp', 'tile')
The draws below stay inside these ranges and needn't reach their ends.
Inputs may be any that keep to these rules, and one draw needn't show every extreme that they name: `remap_dest`: among the 16 entries of one device, each destination device is named at most 2 times.
All inputs are finite; a program needn't handle non-finite values.
Results may differ from the reference program's by a relative error of at most 0.0046.
Values may be sent and summed in bfloat16 or wider, within the bound.
No kernel may reach another device: no remote copies, remote signals or barrier semaphores. Data moves between devices by JAX's collectives and lax.ppermute only.
A program may use at most 64 MiB of HBM per device.

```python
import jax
import jax.numpy as jnp
from jax import lax

BLK = 128
FIELDS = 4
LEV = 60
SURF = 8
SLOTS = 4
HALO = 8
FOLD = 8
STEPS = 2
CAP = 2
DYN_TILES = 64
REMAP_TILES = 64
NB_DEV = 16
RMAP = 16
NBLK = 256
N_TILE = 16


def offsets_of(key):
    rest = jax.random.permutation(key, N_TILE - 1).astype(jnp.int32)
    rest = jnp.where(rest >= 1, rest + 1, rest)
    return jnp.concatenate([jnp.ones((1,), jnp.int32), rest])


def draw_remap_dest(key, part):
    keys = jax.random.split(jax.random.fold_in(key, 7), 2 * N_TILE)
    offsets = jax.vmap(offsets_of)(keys)
    group = jnp.arange(RMAP, dtype=jnp.int32) // CAP
    chosen = offsets[:, group]
    device = (jnp.arange(2 * N_TILE, dtype=jnp.int32) % N_TILE)[:, None]
    dest = (device + chosen) % N_TILE
    return dest.reshape(2, N_TILE * RMAP, 1).astype(jnp.int32)


def plant(drawn, stream_key, least, high):
    place = [jax.random.randint(jax.random.fold_in(stream_key, axis), (), 0, length) for axis, length in enumerate(drawn.shape)]
    widest = drawn.shape.index(max(drawn.shape))
    neighbour = place[:widest] + [(place[widest] + 1) % drawn.shape[widest]] + place[widest + 1:]
    return drawn.at[tuple(place)].set(least).at[tuple(neighbour)].set(high)


def block_scale(rng, shape, pieces, low, largest):
    factor_of = 1.0
    for position, blocks in pieces:
        steps = jax.random.uniform(jax.random.fold_in(jax.random.fold_in(rng, 6), position), (blocks,), jnp.float32, low / len(pieces), largest / len(pieces))
        factor_of = factor_of * jnp.repeat(jnp.exp(steps), shape[position] // blocks).reshape((-1,) + (1,) * (len(shape) - 1 - position))
    return factor_of


def gaussian(rng, extent, spread, bound, cuts=(), kind=jnp.bfloat16):
    drawn = spread * jax.random.normal(rng, extent, jnp.float32)
    if cuts:
        drawn = drawn * block_scale(rng, extent, cuts, -0.22, 0.18)
    return jnp.clip(drawn, -bound, bound).astype(kind)


def setup_inputs(seed: int = 0) -> dict:
    arg_keys = jax.random.split(jax.random.key(seed), 11)
    return {
        "state": gaussian(arg_keys[0], (2, NBLK, FIELDS, LEV, BLK), 1.0, 6.0, ((0, 2), (1, 16))),
        "dyn_weights": gaussian(arg_keys[1], (2, DYN_TILES, BLK, BLK), (2 * BLK * SLOTS) ** -0.5, 0.1875, ((0, 2),)),
        "vertical": gaussian(arg_keys[2], (2, LEV, LEV), LEV ** -0.5, 0.75, ((0, 2),), jnp.float32),
        "remap_weights": gaussian(arg_keys[3], (2, REMAP_TILES, BLK, BLK), BLK ** -0.5, 0.5),
        "neighbor_slots": plant(jax.random.randint(arg_keys[4], (2, NBLK, SLOTS), 0, NB_DEV + 2 * HALO + FOLD), jax.random.fold_in(arg_keys[4], 1), 0, (NB_DEV + 2 * HALO + FOLD) - 1).astype(jnp.int32),
        "neighbor_tiles": plant(jax.random.randint(arg_keys[5], (2, NBLK, SLOTS), 0, DYN_TILES), jax.random.fold_in(arg_keys[5], 1), 0, DYN_TILES - 1).astype(jnp.int32),
        "remap_source": plant(jax.random.randint(arg_keys[6], (2, N_TILE * RMAP), 0, NB_DEV), jax.random.fold_in(arg_keys[6], 1), 0, NB_DEV - 1).astype(jnp.int32),
        "remap_target": plant(jax.random.randint(arg_keys[7], (2, N_TILE * RMAP), 0, NB_DEV), jax.random.fold_in(arg_keys[7], 1), 0, NB_DEV - 1).astype(jnp.int32),
        "remap_tile": plant(jax.random.randint(arg_keys[8], (2, N_TILE * RMAP), 0, REMAP_TILES), jax.random.fold_in(arg_keys[8], 1), 0, REMAP_TILES - 1).astype(jnp.int32),
        "remap_dest": draw_remap_dest(jax.random.fold_in(arg_keys[10], 71), 0),
    }


def global_index(local):
    nblk = NB_DEV * N_TILE
    device = (jnp.arange(nblk, dtype=jnp.int32) // NB_DEV)[:, None]
    before = ((device - 1) % N_TILE) * NB_DEV + NB_DEV - HALO + local
    mine = device * NB_DEV + local - HALO
    after = ((device + 1) % N_TILE) * NB_DEV + local - HALO - NB_DEV
    across = jnp.bitwise_xor(device, N_TILE // 2) * NB_DEV + local - 2 * HALO - NB_DEV
    picked = jnp.where(local < HALO, before, jnp.where(local < HALO + NB_DEV, mine, jnp.where(local < 2 * HALO + NB_DEV, after, across)))
    return picked.astype(jnp.int32)


def advance_interval(operator_blocks, exchange_weights, vertical_matrix, block_positions, tile_indices):
    nblk = NB_DEV * N_TILE
    source = global_index(block_positions)
    for step in range(STEPS):
        flux = jnp.zeros(operator_blocks.shape, jnp.float32)
        for k in range(SLOTS):
            rows = operator_blocks[source[:, k]].astype(jnp.float32)
            tiles_k = exchange_weights[tile_indices[:, k]].astype(jnp.float32)
            flux = flux + jnp.einsum('brc,bcd->brd', rows, tiles_k, precision=lax.Precision.HIGHEST)
        middle_state = (operator_blocks.astype(jnp.float32) + flux).reshape(nblk, FIELDS, LEV, BLK)
        mixed_state = jnp.einsum('se,ivey->ivsy', vertical_matrix, middle_state, precision=lax.Precision.HIGHEST)
        operator_blocks = (middle_state + jnp.tanh(mixed_state)).reshape(nblk, FIELDS * LEV, BLK).astype(jnp.bfloat16)
    return operator_blocks


def reference(state, dyn_weights, vertical, remap_weights, neighbor_slots, neighbor_tiles, remap_source, remap_target, remap_tile, remap_dest):
    nblk = NB_DEV * N_TILE
    finals = []
    for comp in range(2):
        operator_blocks = state[comp].reshape(nblk, FIELDS * LEV, BLK)
        operator_blocks = advance_interval(operator_blocks, dyn_weights[comp], vertical[comp], neighbor_slots[comp], neighbor_tiles[comp])
        finals.append(operator_blocks.reshape(nblk, FIELDS, LEV, BLK))
    entries = remap_source.shape[1]
    owner = jnp.arange(entries, dtype=jnp.int32) // RMAP
    outputs = []
    for comp in range(2):
        other = 1 - comp
        surface = finals[other][:, :, :SURF, :].reshape(nblk, FIELDS * SURF, BLK)
        rows = surface[owner * NB_DEV + remap_source[other]].astype(jnp.float32)
        tile_indices = remap_weights[comp][remap_tile[other]].astype(jnp.float32)
        partial_value = jnp.einsum('erc,ecd->erd', rows, tile_indices, precision=lax.Precision.HIGHEST)
        target = (remap_dest[other, :, 0] * NB_DEV + remap_target[other]).astype(jnp.int32)
        coupled = jax.ops.segment_sum(partial_value, target, num_segments=nblk)
        mine = finals[comp]
        top = (mine[:, :, :SURF, :].astype(jnp.float32) + coupled.reshape(nblk, FIELDS, SURF, BLK)).astype(jnp.bfloat16)
        outputs.append(jnp.concatenate([top, mine[:, :, SURF:, :]], axis=2))
    return jnp.stack(outputs, axis=0)
```

```python
import functools

import jax
import jax.numpy as jnp
from jax import lax
from jax.experimental import pallas as pl
from jax.experimental.pallas import tpu as pltpu
from jax.sharding import PartitionSpec as P

SURF = 8
HALO = 8
FOLD = 8
STEPS = 2
CAP = 2
STAGES = 2

VMEM = pltpu.MemorySpace.VMEM
SMEM = pltpu.MemorySpace.SMEM
HBM = pltpu.MemorySpace.HBM
BF16 = jnp.bfloat16
F32 = jnp.float32


def spec(space):
    return pl.BlockSpec(memory_space=space)


def shape_of(shape, dtype=BF16):
    return jax.ShapeDtypeStruct(shape, dtype)


def params():
    return pltpu.CompilerParams(vmem_limit_bytes=40 * 1024 * 1024)


def cost(flops, moved):
    return pl.CostEstimate(flops=flops, bytes_accessed=moved, transcendentals=0)


def select_matrix(rows, fields, group, first, inverse):
    wide = rows // group * fields
    shape = (wide, rows) if inverse else (rows, wide)
    mine = lax.broadcasted_iota(jnp.int32, shape, 1 if inverse else 0)
    other = lax.broadcasted_iota(jnp.int32, shape, 0 if inverse else 1)
    source = (mine // group) * fields + first + mine % group
    return jnp.where(source == other, 1.0, 0.0).astype(BF16)


def split_kernel(fields, group, first, x, lead, last):
    half = lead.shape[0]
    pick = select_matrix(lead.shape[1], fields, group, first, False)
    for b in range(0, x.shape[0], 2):
        pair = jnp.concatenate([x[b], x[b + 1]], axis=1)
        got = jnp.dot(pick, pair, preferred_element_type=F32).astype(BF16)
        for i in range(2):
            dst, at = (lead, b + i) if b + i < half else (last, b + i - half)
            dst[at] = got[:, i * 128 : (i + 1) * 128]


def step_kernel(slots, tiles, before, lead, last, after, across, w, k_hi, k_lo, *rest):
    outs, (pool, mid, hi, lo, sems) = rest[:-5], rest[-5:]
    final = len(outs) == 2 and outs[0].shape[0] != outs[1].shape[0] or outs[0].shape[1] != outs[1].shape[1]
    copies, at = [], 0
    for i, src in enumerate((before, lead, last, after, across)):
        n = src.shape[0]
        copies.append(pltpu.make_async_copy(src, pool.at[pl.ds(at, n)], sems.at[i]))
        at += n
    for c in copies:
        c.start()
    for c in copies:
        c.wait()
    own = before.shape[0]
    count = lead.shape[0] + last.shape[0]
    entries = slots.shape[0] // count
    width = w.shape[1]
    for b in range(count):
        total = pool[own + b].astype(F32)
        for k in range(0, entries, 2):
            e = b * entries + k
            lhs = jnp.concatenate([pool[slots[e]], pool[slots[e + 1]]], axis=1)
            rhs = jnp.concatenate([w[tiles[e]], w[tiles[e + 1]]], axis=0)
            total = total + jnp.dot(lhs, rhs, preferred_element_type=F32)
        lanes = slice(b * width, (b + 1) * width)
        mid[:, lanes] = total
        top = total.astype(BF16)
        hi[:, lanes] = top
        lo[:, lanes] = (total - top.astype(F32)).astype(BF16)
    big, small = k_hi[...], k_lo[...]
    for b in range(0, count, 2):
        lanes = slice(b * width, (b + 2) * width)
        mixed = jnp.dot(big, hi[:, lanes], preferred_element_type=F32)
        mixed = mixed + jnp.dot(big, lo[:, lanes], preferred_element_type=F32)
        mixed = mixed + jnp.dot(small, hi[:, lanes], preferred_element_type=F32)
        new = (mid[:, lanes] + jnp.tanh(mixed)).astype(BF16)
        for i in range(2):
            piece = new[:, i * width : (i + 1) * width]
            if final:
                outs[0][b + i] = piece
                outs[1][b + i] = piece[: outs[1].shape[1]]
            else:
                half = outs[0].shape[0]
                dst, at = (outs[0], b + i) if b + i < half else (outs[1], b + i - half)
                dst[at] = piece


def run_step(tables, pieces, w, k_hi, k_lo, surface_rows):
    before, lead, last, after, across = pieces
    _, rows, width = lead.shape
    count = lead.shape[0] + last.shape[0]
    total = count + before.shape[0] + after.shape[0] + across.shape[0]
    if surface_rows:
        outs = [shape_of((count, rows, width)), shape_of((count, surface_rows, width))]
    else:
        outs = [shape_of(lead.shape), shape_of(last.shape)]
    return pl.pallas_call(
        step_kernel,
        out_shape=outs,
        in_specs=[spec(SMEM)] * 2 + [spec(HBM)] * 5 + [spec(VMEM)] * 3,
        out_specs=[spec(VMEM)] * 2,
        scratch_shapes=[
            pltpu.VMEM((total, rows, width), BF16),
            pltpu.VMEM((rows, count * width), F32),
            pltpu.VMEM((rows, count * width), BF16),
            pltpu.VMEM((rows, count * width), BF16),
            pltpu.SemaphoreType.DMA((5,)),
        ],
        compiler_params=params(),
        cost_estimate=cost(4 * 2 * count * rows * width * width, 8 * 1024 * 1024),
        name="substep",
    )(*tables, *pieces, w, k_hi, k_lo)


def partial_kernel(source, tile, slot, comp, weights, *rest):
    surfaces, (payload, held, sem) = rest[:-3], rest[-3:]
    entries = source.shape[0]
    copies = [
        pltpu.make_async_copy(weights.at[comp[0], tile[e]], held.at[e], sem.at[e])
        for e in range(entries)
    ]
    for c in copies:
        c.start()
    payload[...] = jnp.zeros(payload.shape, payload.dtype)
    for c in copies:
        c.wait()
    for e in range(entries):
        rows = [s[source[e]] for s in surfaces]
        rows = rows[0] if len(rows) == 1 else jnp.concatenate(rows, axis=0)
        payload[slot[e]] = jnp.dot(rows, held[e], preferred_element_type=F32).astype(BF16)


def merge_kernel(fields, group, *refs):
    stages, out = refs[:-1], refs[-1]
    width = out.shape[2]
    picks = [
        select_matrix(s.shape[1], fields, group, i * group, True) for i, s in enumerate(stages)
    ]
    for b in range(0, out.shape[0], 2):
        got = None
        for pick, s in zip(picks, stages):
            pair = jnp.concatenate([s[b], s[b + 1]], axis=1)
            part = jnp.dot(pick, pair, preferred_element_type=F32)
            got = part if got is None else got + part
        got = got.astype(BF16)
        out[b] = got[:, :width]
        out[b + 1] = got[:, width:]


def couple_kernel(fields, group, targets, state, received, *rest):
    surfaces, (out, total, top, sem) = rest[:-4], rest[-4:]
    del state
    count, rows, _ = total.shape
    total[...] = jnp.zeros(total.shape, F32)
    for j in range(targets.shape[0]):
        t = targets[j]

        @pl.when(t >= 0)
        def _(t=t, j=j):
            total[t] = total[t] + received[j].astype(F32)

    step = rows // len(surfaces)
    picks = [select_matrix(step, fields, group, i * group, True) for i in range(len(surfaces))]
    for b in range(count):
        if len(surfaces) == 1:
            top[b] = (surfaces[0][b].astype(F32) + total[b]).astype(BF16)
        else:
            got = None
            for i, s in enumerate(surfaces):
                new = (s[b].astype(F32) + total[b, i * step : (i + 1) * step]).astype(BF16)
                part = jnp.dot(picks[i], new, preferred_element_type=F32)
                got = part if got is None else got + part
            top[b] = got.astype(BF16)
    copy = pltpu.make_async_copy(top, out.at[:, pl.ds(0, rows)], sem)
    copy.start()
    copy.wait()


def partner(value, axis, distance):
    mask = 2**distance
    pairs = [(source, source ^ mask) for source in range(lax.axis_size(axis))]
    return lax.ppermute(value, axis, pairs)


def exchange(lead, last):
    peers = lax.axis_size("tile")
    up = [(i, (i + 1) % peers) for i in range(peers)]
    down = [(j, i) for i, j in up]
    across = partner(lead, "tile", peers.bit_length() - 2)
    before = lax.ppermute(last, "tile", up)
    after = lax.ppermute(lead, "tile", down)
    return before, after, across


def on_device(
    state,
    dyn_weights,
    vertical,
    remap_weights,
    neighbor_slots,
    neighbor_tiles,
    remap_source,
    remap_target,
    remap_tile,
    remap_dest,
):
    _, count, fields, levels, width = state.shape
    group = fields // STAGES
    rows = levels * group
    tile_count = lax.axis_size("tile")
    comp = lax.axis_index("comp")
    w = dyn_weights[0]
    plain = state[0].transpose(0, 2, 1, 3).reshape(count, levels * fields, width)

    kron = (vertical[0][:, None, :, None] * jnp.eye(group, dtype=F32)[None, :, None, :]).reshape(
        rows, rows
    )
    k_hi = lax.reduce_precision(kron, 8, 7)
    k_lo = (kron - k_hi).astype(BF16)
    k_hi = k_hi.astype(BF16)

    dest = remap_dest[0, :, 0]
    hits = (dest[:, None] == jnp.arange(tile_count, dtype=jnp.int32)[None, :]).astype(jnp.int32)
    rank = jnp.sum((jnp.cumsum(hits, axis=0) - 1) * hits, axis=1)
    slot_of = dest * CAP + rank
    place = jnp.arange(tile_count * CAP, dtype=jnp.int32)[:, None] == slot_of[None, :]
    target_buf = jnp.max(jnp.where(place, remap_target[0][None, :], -1), axis=1)

    stages = []
    for s in range(STAGES):
        if STAGES == 1:
            lead, last = plain[:HALO], plain[HALO:]
        else:
            lead, last = pl.pallas_call(
                functools.partial(split_kernel, fields, group, s * group),
                out_shape=[shape_of((HALO, rows, width)), shape_of((count - HALO, rows, width))],
                in_specs=[spec(VMEM)],
                out_specs=[spec(VMEM)] * 2,
                compiler_params=params(),
                cost_estimate=cost(2 * count * rows * rows * width, 2 * 1024 * 1024),
                name="split",
            )(plain)
        before, after, across = exchange(lead, last)
        stages.append((before, lead, last, after, across))

    targets = partner(target_buf, "comp", 0)
    targets = lax.all_to_all(targets, "tile", split_axis=0, concat_axis=0, tiled=True)
    tables = (neighbor_slots[0].reshape(-1), neighbor_tiles[0].reshape(-1))
    tables, targets = lax.optimization_barrier((tables, targets))

    for step in range(STEPS - 1):
        moved = []
        for pieces in stages:
            lead, last = run_step(tables, pieces, w, k_hi, k_lo, 0)
            before, after, across = exchange(lead, last)
            moved.append((before, lead, last, after, across))
        stages = moved
    ended = [run_step(tables, pieces, w, k_hi, k_lo, SURF * group) for pieces in stages]
    bodies = [e[0] for e in ended]
    surfaces = [e[1] for e in ended]

    entries = remap_source.shape[1]
    surface = SURF * fields
    payload = pl.pallas_call(
        partial_kernel,
        out_shape=shape_of((tile_count * CAP, surface, width)),
        in_specs=[spec(SMEM)] * 4 + [spec(HBM)] + [spec(VMEM)] * STAGES,
        out_specs=spec(VMEM),
        scratch_shapes=[
            pltpu.VMEM((entries, width, width), BF16),
            pltpu.SemaphoreType.DMA((entries,)),
        ],
        compiler_params=params(),
        cost_estimate=cost(2 * entries * surface * width * width, 2 * 1024 * 1024),
        name="partials",
    )(remap_source[0], remap_tile[0], slot_of, (1 - comp).reshape(1), remap_weights, *surfaces)

    payload = partner(payload, "comp", 0).reshape(tile_count, CAP * surface, width)
    received = lax.all_to_all(payload, "tile", split_axis=0, concat_axis=0, tiled=True)
    received = received.reshape(tile_count * CAP, surface, width)

    if STAGES == 1:
        whole = bodies[0]
    else:
        whole = pl.pallas_call(
            functools.partial(merge_kernel, fields, group),
            out_shape=shape_of((count, levels * fields, width)),
            in_specs=[spec(VMEM)] * STAGES,
            out_specs=spec(VMEM),
            compiler_params=params(),
            cost_estimate=cost(2 * count * rows * rows * width, 2 * 1024 * 1024),
            name="merge",
        )(*bodies)
    final = pl.pallas_call(
        functools.partial(couple_kernel, fields, group),
        out_shape=shape_of(whole.shape),
        in_specs=[spec(SMEM), spec(HBM), spec(VMEM)] + [spec(VMEM)] * STAGES,
        out_specs=spec(HBM),
        input_output_aliases={1: 0},
        scratch_shapes=[
            pltpu.VMEM((count, surface, width), F32),
            pltpu.VMEM((count, surface, width), BF16),
            pltpu.SemaphoreType.DMA,
        ],
        compiler_params=params(),
        cost_estimate=cost(1024, 1024 * 1024),
        name="couple",
    )(targets, whole, received, *surfaces)
    return final.reshape(count, levels, fields, width).transpose(0, 2, 1, 3)[None]


def solution(mesh):
    return jax.shard_map(
        on_device,
        mesh=mesh,
        in_specs=(
            P("comp", "tile", None, None, None),
            P("comp", None, None, None),
            P("comp", None, None),
            P(),
            P("comp", "tile", None),
            P("comp", "tile", None),
            P("comp", "tile"),
            P("comp", "tile"),
            P("comp", "tile"),
            P("comp", "tile", None),
        ),
        out_specs=P("comp", "tile", None, None, None),
        check_vma=False,
    )
```

```python
import functools

import jax
import jax.numpy as jnp
from jax import lax
from jax.experimental import pallas as pl
from jax.experimental.pallas import tpu as pltpu
from jax.sharding import PartitionSpec as P

SURF = 8
HALO = 8
FOLD = 8
STEPS = 2
CAP = 2
HEAD = 8
STAGES = 2

VMEM = pltpu.MemorySpace.VMEM
SMEM = pltpu.MemorySpace.SMEM
HBM = pltpu.MemorySpace.HBM
BF16 = jnp.bfloat16
F32 = jnp.float32


def spec(space):
    return pl.BlockSpec(memory_space=space)


def shape_of(shape, dtype=BF16):
    return jax.ShapeDtypeStruct(shape, dtype)


def params():
    return pltpu.CompilerParams(vmem_limit_bytes=40 * 1024 * 1024)


def cost(flops, moved):
    return pl.CostEstimate(flops=flops, bytes_accessed=moved, transcendentals=0)


def select_matrix(rows, fields, group, first, inverse):
    wide = rows // group * fields
    shape = (wide, rows) if inverse else (rows, wide)
    mine = lax.broadcasted_iota(jnp.int32, shape, 1 if inverse else 0)
    other = lax.broadcasted_iota(jnp.int32, shape, 0 if inverse else 1)
    source = (mine // group) * fields + first + mine % group
    return jnp.where(source == other, 1.0, 0.0).astype(BF16)


def expand_kernel(group, v, k_hi, k_lo):
    rows, levels = k_hi.shape[0], v.shape[0]
    shape = (rows, levels)
    level = lax.broadcasted_iota(jnp.int32, shape, 0) // group
    spread = jnp.where(level == lax.broadcasted_iota(jnp.int32, shape, 1), 1.0, 0.0).astype(BF16)
    square = (rows, rows)
    same = (
        lax.broadcasted_iota(jnp.int32, square, 0) % group
        == lax.broadcasted_iota(jnp.int32, square, 1) % group
    )
    value = v[...]
    high = value.astype(BF16)
    low = (value - high.astype(F32)).astype(BF16)
    for part, out in ((high, k_hi), (low, k_lo)):
        tall = jnp.dot(spread, part, preferred_element_type=F32).astype(BF16)
        full = lax.dot_general(
            tall, spread, (((1,), (1,)), ((), ())), preferred_element_type=F32
        )
        out[...] = jnp.where(same, full, 0.0).astype(BF16)


def gather_kernel(tile, comp, weights, held, sem):
    entries = held.shape[0]
    copies = [
        pltpu.make_async_copy(weights.at[comp[0], tile[e]], held.at[e], sem.at[e])
        for e in range(entries)
    ]
    for c in copies:
        c.start()
    for c in copies:
        c.wait()


def split_kernel(fields, group, first, x, lead, last):
    half = lead.shape[0]
    pick = select_matrix(lead.shape[1], fields, group, first, False)
    for b in range(0, x.shape[0], 2):
        pair = jnp.concatenate([x[b], x[b + 1]], axis=1)
        got = jnp.dot(pick, pair, preferred_element_type=F32).astype(BF16)
        for i in range(2):
            dst, at = (lead, b + i) if b + i < half else (last, b + i - half)
            dst[at] = got[:, i * 128 : (i + 1) * 128]


def step_kernel(slots, tiles, before, lead, last, after, across, w, k_hi, k_lo, *rest):
    outs, (pool, mid, hi, lo, sems) = rest[:-5], rest[-5:]
    final = len(outs) == 2 and outs[0].shape[0] != outs[1].shape[0] or outs[0].shape[1] != outs[1].shape[1]
    copies, at = [], 0
    for i, src in enumerate((before, lead, last, after, across)):
        n = src.shape[0]
        copies.append(pltpu.make_async_copy(src, pool.at[pl.ds(at, n)], sems.at[i]))
        at += n
    for c in copies:
        c.start()
    for c in copies:
        c.wait()
    own = before.shape[0]
    count = lead.shape[0] + last.shape[0]
    entries = slots.shape[0] // count
    width = w.shape[1]
    for b in range(count):
        total = pool[own + b].astype(F32)
        for k in range(0, entries, 2):
            e = b * entries + k
            lhs = jnp.concatenate([pool[slots[e]], pool[slots[e + 1]]], axis=1)
            rhs = jnp.concatenate([w[tiles[e]], w[tiles[e + 1]]], axis=0)
            total = total + jnp.dot(lhs, rhs, preferred_element_type=F32)
        lanes = slice(b * width, (b + 1) * width)
        mid[:, lanes] = total
        top = total.astype(BF16)
        hi[:, lanes] = top
        lo[:, lanes] = (total - top.astype(F32)).astype(BF16)
    big, small = k_hi[...], k_lo[...]
    for b in range(0, count, 2):
        lanes = slice(b * width, (b + 2) * width)
        mixed = jnp.dot(big, hi[:, lanes], preferred_element_type=F32)
        mixed = mixed + jnp.dot(big, lo[:, lanes], preferred_element_type=F32)
        mixed = mixed + jnp.dot(small, hi[:, lanes], preferred_element_type=F32)
        new = (mid[:, lanes] + jnp.tanh(mixed)).astype(BF16)
        for i in range(2):
            piece = new[:, i * width : (i + 1) * width]
            if final:
                outs[0][b + i] = piece
                outs[1][b + i] = piece[: outs[1].shape[1]]
            else:
                half = outs[0].shape[0]
                dst, at = (outs[0], b + i) if b + i < half else (outs[1], b + i - half)
                dst[at] = piece


def run_step(tables, pieces, w, k_hi, k_lo, surface_rows):
    before, lead, last, after, across = pieces
    _, rows, width = lead.shape
    count = lead.shape[0] + last.shape[0]
    total = count + before.shape[0] + after.shape[0] + across.shape[0]
    if surface_rows:
        outs = [shape_of((count, rows, width)), shape_of((count, surface_rows, width))]
    else:
        outs = [shape_of(lead.shape), shape_of(last.shape)]
    return pl.pallas_call(
        step_kernel,
        out_shape=outs,
        in_specs=[spec(SMEM)] * 2 + [spec(HBM)] * 5 + [spec(VMEM)] * 3,
        out_specs=[spec(VMEM)] * 2,
        scratch_shapes=[
            pltpu.VMEM((total, rows, width), BF16),
            pltpu.VMEM((rows, count * width), F32),
            pltpu.VMEM((rows, count * width), BF16),
            pltpu.VMEM((rows, count * width), BF16),
            pltpu.SemaphoreType.DMA((5,)),
        ],
        compiler_params=params(),
        cost_estimate=cost(4 * 2 * count * rows * width * width, 8 * 1024 * 1024),
        name="substep",
    )(*tables, *pieces, w, k_hi, k_lo)


def partial_kernel(source, slot, header, held, *rest):
    surfaces, payload = rest[:-1], rest[-1]
    surface = sum(s.shape[1] for s in surfaces)
    payload[...] = jnp.zeros(payload.shape, payload.dtype)
    payload[:, CAP * surface :, :] = header[...]
    for e in range(source.shape[0]):
        rows = [s[source[e]] for s in surfaces]
        rows = rows[0] if len(rows) == 1 else jnp.concatenate(rows, axis=0)
        value = jnp.dot(rows, held[e], preferred_element_type=F32).astype(BF16)
        at = pl.multiple_of((slot[e] % CAP) * surface, surface)
        payload[slot[e] // CAP, pl.ds(at, surface), :] = value


def merge_kernel(fields, group, *refs):
    stages, out = refs[:-1], refs[-1]
    width = out.shape[2]
    picks = [
        select_matrix(s.shape[1], fields, group, i * group, True) for i, s in enumerate(stages)
    ]
    for b in range(0, out.shape[0], 2):
        got = None
        for pick, s in zip(picks, stages):
            pair = jnp.concatenate([s[b], s[b + 1]], axis=1)
            part = jnp.dot(pick, pair, preferred_element_type=F32)
            got = part if got is None else got + part
        got = got.astype(BF16)
        out[b] = got[:, :width]
        out[b + 1] = got[:, width:]


def couple_kernel(fields, group, state, received, *rest):
    surfaces, (out, total, top, found, targets, sem) = rest[:-6], rest[-6:]
    del state
    count, rows, width = total.shape
    heads = received[:, CAP * rows :, :].astype(F32)
    found[...] = jnp.sum(heads, axis=0).astype(jnp.int32)
    copy = pltpu.make_async_copy(found, targets, sem)
    copy.start()
    total[...] = jnp.zeros(total.shape, F32)
    copy.wait()
    for j in range(received.shape[0] * CAP):
        t = targets[j // width, j % width]

        @pl.when(t > 0)
        def _(t=t, j=j):
            at = (j % CAP) * rows
            total[t - 1] = total[t - 1] + received[j // CAP, at : at + rows, :].astype(F32)

    step = rows // len(surfaces)
    picks = [select_matrix(step, fields, group, i * group, True) for i in range(len(surfaces))]
    for b in range(count):
        if len(surfaces) == 1:
            top[b] = (surfaces[0][b].astype(F32) + total[b]).astype(BF16)
        else:
            got = None
            for i, s in enumerate(surfaces):
                new = (s[b].astype(F32) + total[b, i * step : (i + 1) * step]).astype(BF16)
                part = jnp.dot(picks[i], new, preferred_element_type=F32)
                got = part if got is None else got + part
            top[b] = got.astype(BF16)
    copy = pltpu.make_async_copy(top, out.at[:, pl.ds(0, rows)], sem)
    copy.start()
    copy.wait()


def partner(value, axis, distance):
    mask = 2**distance
    pairs = [(source, source ^ mask) for source in range(lax.axis_size(axis))]
    return lax.ppermute(value, axis, pairs)


def exchange(lead, last):
    peers = lax.axis_size("tile")
    up = [(i, (i + 1) % peers) for i in range(peers)]
    down = [(j, i) for i, j in up]
    across = partner(lead, "tile", peers.bit_length() - 2)
    before = lax.ppermute(last, "tile", up)
    after = lax.ppermute(lead, "tile", down)
    return before, after, across


def on_device(
    state,
    dyn_weights,
    vertical,
    remap_weights,
    neighbor_slots,
    neighbor_tiles,
    remap_source,
    remap_target,
    remap_tile,
    remap_dest,
):
    _, count, fields, levels, width = state.shape
    group = fields // STAGES
    rows = levels * group
    tile_count = lax.axis_size("tile")
    comp = lax.axis_index("comp")
    w = dyn_weights[0]
    plain = state[0].transpose(0, 2, 1, 3).reshape(count, levels * fields, width)

    k_hi, k_lo = pl.pallas_call(
        functools.partial(expand_kernel, group),
        out_shape=[shape_of((rows, rows))] * 2,
        in_specs=[spec(VMEM)],
        out_specs=[spec(VMEM)] * 2,
        compiler_params=params(),
        cost_estimate=cost(8 * rows * rows * levels, 1024 * 1024),
        name="expand",
    )(vertical[0])

    dest = remap_dest[0, :, 0]
    hits = (dest[:, None] == jnp.arange(tile_count, dtype=jnp.int32)[None, :]).astype(jnp.int32)
    rank = jnp.sum((jnp.cumsum(hits, axis=0) - 1) * hits, axis=1)
    slot_of = dest * CAP + rank
    place = jnp.arange(tile_count * CAP, dtype=jnp.int32)[:, None] == slot_of[None, :]
    target_buf = jnp.max(jnp.where(place, remap_target[0][None, :], -1), axis=1)

    entries = remap_source.shape[1]
    mine = lax.axis_index("tile") * CAP
    flat = jnp.arange(HEAD * width, dtype=jnp.int32).reshape(1, HEAD, width) - mine
    header = jnp.zeros((tile_count, HEAD, width), jnp.int32)
    for i in range(CAP):
        mark = target_buf.reshape(tile_count, CAP)[:, i][:, None, None] + 1
        header = jnp.where(flat == i, mark, header)
    header = header.astype(F32).astype(BF16)
    held = pl.pallas_call(
        gather_kernel,
        out_shape=shape_of((entries, width, width)),
        in_specs=[spec(SMEM)] * 2 + [spec(HBM)],
        out_specs=spec(VMEM),
        scratch_shapes=[pltpu.SemaphoreType.DMA((entries,))],
        compiler_params=params(),
        cost_estimate=cost(1024, 1024 * 1024),
        name="tiles",
    )(remap_tile[0], (1 - comp).reshape(1), remap_weights)

    stages = []
    for s in range(STAGES):
        if STAGES == 1:
            lead, last = plain[:HALO], plain[HALO:]
        else:
            lead, last = pl.pallas_call(
                functools.partial(split_kernel, fields, group, s * group),
                out_shape=[shape_of((HALO, rows, width)), shape_of((count - HALO, rows, width))],
                in_specs=[spec(VMEM)],
                out_specs=[spec(VMEM)] * 2,
                compiler_params=params(),
                cost_estimate=cost(2 * count * rows * rows * width, 2 * 1024 * 1024),
                name="split",
            )(plain)
        before, after, across = exchange(lead, last)
        stages.append((before, lead, last, after, across))

    tables = (neighbor_slots[0].reshape(-1), neighbor_tiles[0].reshape(-1))
    tables, held, header, slot_of = lax.optimization_barrier((tables, held, header, slot_of))

    for step in range(STEPS - 1):
        moved = []
        for pieces in stages:
            lead, last = run_step(tables, pieces, w, k_hi, k_lo, 0)
            before, after, across = exchange(lead, last)
            moved.append((before, lead, last, after, across))
        stages = moved
    ended = [run_step(tables, pieces, w, k_hi, k_lo, SURF * group) for pieces in stages]
    bodies = [e[0] for e in ended]
    surfaces = [e[1] for e in ended]

    surface = SURF * fields
    payload = pl.pallas_call(
        partial_kernel,
        out_shape=shape_of((tile_count, CAP * surface + HEAD, width)),
        in_specs=[spec(SMEM)] * 2 + [spec(VMEM)] * (2 + STAGES),
        out_specs=spec(VMEM),
        compiler_params=params(),
        cost_estimate=cost(2 * entries * surface * width * width, 2 * 1024 * 1024),
        name="partials",
    )(remap_source[0], slot_of, header, held, *surfaces)

    payload = partner(payload, "comp", 0)
    received = lax.all_to_all(payload, "tile", split_axis=0, concat_axis=0, tiled=True)

    if STAGES == 1:
        whole = bodies[0]
    else:
        whole = pl.pallas_call(
            functools.partial(merge_kernel, fields, group),
            out_shape=shape_of((count, levels * fields, width)),
            in_specs=[spec(VMEM)] * STAGES,
            out_specs=spec(VMEM),
            compiler_params=params(),
            cost_estimate=cost(2 * count * rows * rows * width, 2 * 1024 * 1024),
            name="merge",
        )(*bodies)
    final = pl.pallas_call(
        functools.partial(couple_kernel, fields, group),
        out_shape=shape_of(whole.shape),
        in_specs=[spec(HBM), spec(VMEM)] + [spec(VMEM)] * STAGES,
        out_specs=spec(HBM),
        input_output_aliases={0: 0},
        scratch_shapes=[
            pltpu.VMEM((count, surface, width), F32),
            pltpu.VMEM((count, surface, width), BF16),
            pltpu.VMEM((HEAD, width), jnp.int32),
            pltpu.SMEM((HEAD, width), jnp.int32),
            pltpu.SemaphoreType.DMA,
        ],
        compiler_params=params(),
        cost_estimate=cost(1024, 1024 * 1024),
        name="couple",
    )(whole, received, *surfaces)
    return final.reshape(count, levels, fields, width).transpose(0, 2, 1, 3)[None]


def solution(mesh):
    return jax.shard_map(
        on_device,
        mesh=mesh,
        in_specs=(
            P("comp", "tile", None, None, None),
            P("comp", None, None, None),
            P("comp", None, None),
            P(),
            P("comp", "tile", None),
            P("comp", "tile", None),
            P("comp", "tile"),
            P("comp", "tile"),
            P("comp", "tile"),
            P("comp", "tile", None),
        ),
        out_specs=P("comp", "tile", None, None, None),
        check_vma=False,
    )
```

```python
import functools

import jax
import jax.numpy as jnp
from jax import lax
from jax.experimental import pallas as pl
from jax.experimental.pallas import tpu as pltpu
from jax.sharding import PartitionSpec as P


SURF = 8
HALO = 8
STEPS = 2
CAP = 2
HEAD = 8

VMEM = pltpu.MemorySpace.VMEM
SMEM = pltpu.MemorySpace.SMEM
HBM = pltpu.MemorySpace.HBM
BF16 = jnp.bfloat16
F32 = jnp.float32
I32 = jnp.int32


def spec(space):
    return pl.BlockSpec(memory_space=space)


def shape_of(shape, dtype=BF16):
    return jax.ShapeDtypeStruct(shape, dtype)


def params():
    return pltpu.CompilerParams(vmem_limit_bytes=16 * 1024 * 1024)


def cost(flops, moved):
    return pl.CostEstimate(flops=flops, bytes_accessed=moved, transcendentals=0)


def select_matrix(rows, wide, fields, group, first, inverse):
    shape = (wide, rows) if inverse else (rows, wide)
    mine = lax.broadcasted_iota(I32, shape, 1 if inverse else 0)
    other = lax.broadcasted_iota(I32, shape, 0 if inverse else 1)
    source = (mine // group) * fields + first + mine % group
    return jnp.where(source == other, 1.0, 0.0).astype(BF16)


def expand_kernel(group, v, k_hi, k_lo):
    rows, levels = k_hi.shape[0], v.shape[0]
    shape = (rows, levels)
    level = lax.broadcasted_iota(I32, shape, 0) // group
    spread = jnp.where(level == lax.broadcasted_iota(I32, shape, 1), 1.0, 0.0).astype(BF16)
    square = (rows, rows)
    same = (
        lax.broadcasted_iota(I32, square, 0) % group == lax.broadcasted_iota(I32, square, 1) % group
    )
    value = v[...]
    high = value.astype(BF16)
    low = (value - high.astype(F32)).astype(BF16)
    for part, out in ((high, k_hi), (low, k_lo)):
        tall = jnp.dot(spread, part, preferred_element_type=F32).astype(BF16)
        full = lax.dot_general(tall, spread, (((1,), (1,)), ((), ())), preferred_element_type=F32)
        out[...] = jnp.where(same, full, 0.0).astype(BF16)


def table_kernel(slots, tiles, *rest):
    singles, table = rest[:-1], rest[-1]
    at = 0
    for src in (slots, tiles, *singles):
        for i in range(src.shape[0]):
            for j in range(src.shape[1]):
                table[at] = src[i, j]
                at += 1


def route_kernel(size, entries, ids, own, far, weights, held, slot, header, marks, taken, sem):
    peers = header.shape[0]
    copies = []
    for x, table in enumerate((own, far)):
        for e in range(entries):
            src = weights.at[1 - ids[1], table[2 * size + entries + e]]
            copies.append(pltpu.make_async_copy(src, held.at[x * entries + e], sem.at[x * entries + e]))
    for c in copies:
        c.start()
    for x, table in enumerate((own, far)):
        for p in range(peers):
            taken[p] = 0
            for i in range(CAP):
                marks[p * 2 * CAP + x * CAP + i] = 0
        for e in range(entries):
            dest = table[2 * size + 2 * entries + e]
            rank = taken[dest]
            taken[dest] = rank + 1
            slot[x * entries + e] = dest * CAP + rank
            marks[dest * 2 * CAP + x * CAP + rank] = table[2 * size + 3 * entries + e] + 1
    shape = header.shape[1:]
    flat = lax.broadcasted_iota(I32, shape, 0) * shape[1] + lax.broadcasted_iota(I32, shape, 1)
    flat = flat - ids[0] * 2 * CAP
    for p in range(peers):
        value = jnp.zeros(shape, I32)
        for i in range(2 * CAP):
            value = jnp.where(flat == i, marks[p * 2 * CAP + i], value)
        header[p] = value.astype(F32).astype(BF16)
    for c in copies:
        c.wait()


def far_fields(near_group, far_group, ring, ids):
    is_low = jnp.where(ids[0] < ring, 1, 0)
    return near_group + is_low * far_group, near_group + (1 - is_low) * far_group


def split_kernel(fields, near_group, far_group, ring, ids, x, lead, last, sent, kept):
    half, rows, width = lead.shape
    wide = x.shape[1]
    near = select_matrix(rows, wide, fields, near_group, 0, False)
    first = far_fields(near_group, far_group, ring, ids)
    far = [select_matrix(sent.shape[1], wide, fields, far_group, f, False) for f in first]
    for b in range(0, x.shape[0], 2):
        pair = jnp.concatenate([x[b], x[b + 1]], axis=1)
        for pick, outs in zip((near, *far), ((lead, last), (sent,), (kept,))):
            got = jnp.dot(pick, pair, preferred_element_type=F32).astype(BF16)
            for i in range(2):
                dst, at = (outs[0], b + i) if b + i < outs[0].shape[0] else (outs[1], b + i - half)
                dst[at] = got[:, i * width : (i + 1) * width]


def pack_kernel(mine, other, leads, lasts):
    half = leads.shape[0] // 2
    for i, src in enumerate((mine, other)):
        leads[pl.ds(i * half, half)] = src[pl.ds(0, half)]
        lasts[pl.ds(i * half, half)] = src[pl.ds(half, half)]


def far_index(slot, x, at, ring, count):
    side_before = jnp.where(at == 0, 1 - x, x)
    side_after = jnp.where(at == ring - 1, 1 - x, x)
    inner = slot - HALO
    later = inner - count
    home = jnp.where(inner < HALO, x * HALO + inner, HALO + x * HALO + inner)
    beyond = jnp.where(
        later < HALO, 3 * count + side_after * HALO + later, (1 - x) * HALO + later - HALO
    )
    inside = jnp.where(inner < count, home, beyond)
    return jnp.where(inner < 0, 2 * count + side_before * HALO + slot, inside)


def step_kernel(pieces, size, ring, own_at, writes, ids, own, far, *refs):
    sources, (w, k_hi, k_lo) = refs[:pieces], refs[pieces : pieces + 3]
    outs, (pool, mid, hi, lo) = refs[pieces + 3 : -4], refs[-4:]
    at = 0
    for src in sources:
        n = src.shape[0]
        pool[pl.ds(at, n)] = src[...]
        at += n
    count = len(own_at)
    stride = count // 2 if ring else count
    width = w.shape[1]
    for b in range(count):
        total = pool[own_at[b]].astype(F32)
        x, table = b // stride, far if b >= stride else own
        entries = range(b % stride, size, stride)
        where = [table[e] for e in entries]
        if ring:
            where = [far_index(slot, x, ids[0] % ring, ring, stride) for slot in where]
        what = [table[size + e] for e in entries]
        for k in range(0, len(what), 2):
            lhs = jnp.concatenate([pool[where[k]], pool[where[k + 1]]], axis=1)
            rhs = jnp.concatenate([w[what[k]], w[what[k + 1]]], axis=0)
            total = total + jnp.dot(lhs, rhs, preferred_element_type=F32)
        lanes = slice(b * width, (b + 1) * width)
        mid[:, lanes] = total
        top = total.astype(BF16)
        hi[:, lanes] = top
        lo[:, lanes] = (total - top.astype(F32)).astype(BF16)
    big, small = k_hi[...], k_lo[...]
    for b in range(0, count, 2):
        lanes = slice(b * width, (b + 2) * width)
        mixed = jnp.dot(big, hi[:, lanes], preferred_element_type=F32)
        mixed = mixed + jnp.dot(big, lo[:, lanes], preferred_element_type=F32)
        mixed = mixed + jnp.dot(small, hi[:, lanes], preferred_element_type=F32)
        new = (mid[:, lanes] + jnp.tanh(mixed)).astype(BF16)
        for i in range(2):
            for out, place, rows in writes[b + i]:
                outs[out][place] = new[:rows, i * width : (i + 1) * width]


def run_step(size, ring, tables, pieces, w, k, own_at, outs, writes):
    _, rows, width = pieces[0].shape
    count = len(own_at)
    total = sum(p.shape[0] for p in pieces)
    return pl.pallas_call(
        functools.partial(step_kernel, len(pieces), size, ring, own_at, writes),
        out_shape=[shape_of(o) for o in outs],
        in_specs=[spec(SMEM)] * 3 + [spec(VMEM)] * len(pieces) + [spec(VMEM)] * 3,
        out_specs=[spec(VMEM)] * len(outs),
        scratch_shapes=[
            pltpu.VMEM((total, rows, width), BF16),
            pltpu.VMEM((rows, count * width), F32),
            pltpu.VMEM((rows, count * width), BF16),
            pltpu.VMEM((rows, count * width), BF16),
        ],
        compiler_params=params(),
        cost_estimate=cost(4 * 2 * count * rows * width * width, 8 * 1024 * 1024),
    )(*tables, *pieces, w, *k)


def partial_kernel(size, own, far, slot, header, held, near, mine, other, payload):
    entries = slot.shape[0] // 2
    wide = (near.shape[1] + mine.shape[1]) // 8
    thin = other.shape[1] // 8
    payload[...] = jnp.zeros(payload.shape, payload.dtype)
    payload[:, payload.shape[1] - HEAD // 8] = header[...]
    for e in range(2 * entries):
        src = (own if e < entries else far)[2 * size + e % entries]
        groups, base = thin, CAP * wide
        if e < entries:
            rows, groups, base = jnp.concatenate([near[src], mine[src]], axis=0), wide, 0
        else:
            rows = other[src]
        value = jnp.dot(rows, held[e], preferred_element_type=F32)
        value = value.reshape(groups, 8, value.shape[1]).astype(BF16)
        payload[slot[e] // CAP, pl.ds(base + (slot[e] % CAP) * groups, groups)] = value


def merge_kernel(fields, near_group, far_group, ring, ids, near, mine, other, out):
    _, wide, width = out.shape
    first = far_fields(near_group, far_group, ring, ids)
    picks = [
        select_matrix(near.shape[1], wide, fields, near_group, 0, True),
        select_matrix(mine.shape[1], wide, fields, far_group, first[1], True),
        select_matrix(mine.shape[1], wide, fields, far_group, first[0], True),
    ]
    for b in range(0, out.shape[0], 2):
        got = None
        for pick, s in zip(picks, (near, mine, other)):
            pair = jnp.concatenate([s[b], s[b + 1]], axis=1)
            part = jnp.dot(pick, pair, preferred_element_type=F32)
            got = part if got is None else got + part
        got = got.astype(BF16)
        out[b] = got[:, :width]
        out[b + 1] = got[:, width:]


def couple_kernel(
    fields, near_group, far_group, ids, state, received, near, mine, other, out, *scratch
):
    total, top, found, targets, sem = scratch
    del state
    count, rows, width = top.shape
    peers = received.shape[0]
    close, far = near.shape[1], mine.shape[1]
    wide, thin = (close + far) // 8, far // 8
    heads = received[:, received.shape[1] - HEAD // 8].astype(F32)
    found[...] = jnp.sum(heads, axis=0).astype(I32)
    copy = pltpu.make_async_copy(found, targets, sem)
    copy.start()
    total[...] = jnp.zeros(total.shape, F32)
    copy.wait()
    for p in range(peers):
        side = close if p < peers // 2 else close + far
        for i in range(2 * CAP):
            q = p * 2 * CAP + i
            t = targets[q // width, q % width]
            if i < CAP:
                got = received[p, i * wide : (i + 1) * wide].astype(F32)
                got = got.reshape(close + far, width)
                total[t, :close] = total[t, :close] + got[:close]
                total[t, side : side + far] = total[t, side : side + far] + got[close:]
            else:
                at = CAP * wide + (i - CAP) * thin
                got = received[p, at : at + thin].astype(F32).reshape(far, width)
                total[t, side : side + far] = total[t, side : side + far] + got
    shape = (rows, rows)
    have = lax.broadcasted_iota(I32, shape, 1)
    a, b = have - close, have - close - far
    want = jnp.where(
        have < close,
        (have // near_group) * fields + have % near_group,
        jnp.where(
            have < close + far,
            (a // far_group) * fields + near_group + a % far_group,
            (b // far_group) * fields + near_group + far_group + b % far_group,
        ),
    )
    pick = jnp.where(want == lax.broadcasted_iota(I32, shape, 0), 1.0, 0.0).astype(BF16)
    is_low = ids[0] < peers // 2
    for g in range(count):
        here = mine[g].astype(F32)
        there = other[g, :far].astype(F32)
        base = jnp.concatenate(
            [near[g].astype(F32), jnp.where(is_low, here, there), jnp.where(is_low, there, here)],
            axis=0,
        )
        new = (base + total[g + 1]).astype(BF16)
        top[g] = jnp.dot(pick, new, preferred_element_type=F32).astype(BF16)
    copy = pltpu.make_async_copy(top, out.at[:, pl.ds(0, rows)], sem)
    copy.start()
    copy.wait()


def partner(value, axis, distance):
    mask = 2**distance
    pairs = [(source, source ^ mask) for source in range(lax.axis_size(axis))]
    return lax.ppermute(value, axis, pairs)


def shift(last, lead, ring):
    peers = lax.axis_size("tile")
    up = [(i, i // ring * ring + (i + 1) % ring) for i in range(peers)]
    down = [(j, i) for i, j in up]
    before = lax.ppermute(last, "tile", up)
    return before, lax.ppermute(lead, "tile", down)


def on_device(
    state,
    dyn_weights,
    vertical,
    remap_weights,
    neighbor_slots,
    neighbor_tiles,
    remap_source,
    remap_target,
    remap_tile,
    remap_dest,
):
    _, count, fields, levels, width = state.shape
    near_group = fields // 2
    far_group = (fields - near_group) // 2
    near_rows = levels * near_group
    far_rows = -(-levels * far_group // 16) * 16
    peers = lax.axis_size("tile")
    ring = peers // 2
    fold_bit = peers.bit_length() - 2
    ids = jnp.stack([lax.axis_index("tile"), lax.axis_index("comp")])
    w = dyn_weights[0]
    plain = state[0].transpose(0, 2, 1, 3).reshape(count, levels * fields, width)

    lead, last, sent, mine = pl.pallas_call(
        functools.partial(split_kernel, fields, near_group, far_group, ring),
        out_shape=[
            shape_of((HALO, near_rows, width)),
            shape_of((count - HALO, near_rows, width)),
            shape_of((count, far_rows, width)),
            shape_of((count, far_rows, width)),
        ],
        in_specs=[spec(SMEM), spec(VMEM)],
        out_specs=[spec(VMEM)] * 4,
        compiler_params=params(),
        cost_estimate=cost(4 * count * near_rows * levels * fields * width, 2 * 1024 * 1024),
        name="split",
    )(ids, plain)
    other = partner(sent, "tile", fold_bit)
    across = partner(lead, "tile", fold_bit)
    before, after = shift(last, lead, peers)

    lists = (neighbor_slots[0].T, neighbor_tiles[0].T, remap_source, remap_tile, remap_dest[:, :, 0], remap_target)
    size, entries = lists[0].size, remap_source.shape[1]
    own_table = pl.pallas_call(
        table_kernel,
        out_shape=shape_of((2 * size + 4 * entries,), I32),
        in_specs=[spec(SMEM)] * len(lists),
        out_specs=spec(SMEM),
        name="table",
    )(*lists)
    far_table = partner(own_table, "tile", fold_bit)

    leads, lasts = pl.pallas_call(
        pack_kernel,
        out_shape=[shape_of((count, far_rows, width))] * 2,
        in_specs=[spec(VMEM)] * 2,
        out_specs=[spec(VMEM)] * 2,
        compiler_params=params(),
        cost_estimate=cost(1024, 1024 * 1024),
        name="pack",
    )(mine, other)

    k_near, k_far = (
        pl.pallas_call(
            functools.partial(expand_kernel, group),
            out_shape=[shape_of((rows, rows))] * 2,
            in_specs=[spec(VMEM)],
            out_specs=[spec(VMEM)] * 2,
            compiler_params=params(),
            cost_estimate=cost(8 * rows * rows * levels, 1024 * 1024),
            name="expand",
        )(vertical[0])
        for group, rows in ((near_group, near_rows), (far_group, far_rows))
    )
    tables = (ids, own_table, far_table)
    tail = 2 * HALO
    tables, k_near, k_far = lax.optimization_barrier((tables, k_near, k_far))
    near_at = tuple(HALO + b for b in range(count))
    far_at = tuple(
        x * HALO + i if i < HALO else tail + x * (count - HALO) + i - HALO
        for x in range(2)
        for i in range(count)
    )
    for step in range(STEPS):
        prior, following = shift(lasts, leads, ring)
        if step < STEPS - 1:
            near_pieces = (before, lead, last, after, across)
            far_pieces = (leads, lasts, prior, following)
            leads, lasts = run_step(
                size, ring, tables, far_pieces, w, k_far, far_at, [leads.shape, lasts.shape],
                [((i % count >= HALO, p if i % count < HALO else p - tail, far_rows),) for i, p in enumerate(far_at)],
            )
            lead, last = run_step(
                size, 0, tables, near_pieces, w, k_near, near_at, [lead.shape, last.shape],
                [((i >= HALO, i % HALO, near_rows),) for i in range(count)],
            )
            across = partner(lead, "tile", fold_bit)
            before, after = shift(last, lead, peers)
    tables, lead, leads = lax.optimization_barrier((tables, lead, leads))
    route = pl.pallas_call(
        functools.partial(route_kernel, size, entries),
        out_shape=[
            shape_of((2 * entries, width, width)),
            shape_of((2 * entries,), I32),
            shape_of((peers, HEAD, width)),
        ],
        in_specs=[spec(SMEM)] * 3 + [spec(HBM)],
        out_specs=[spec(VMEM), spec(SMEM), spec(VMEM)],
        scratch_shapes=[
            pltpu.SMEM((2 * CAP * peers,), I32),
            pltpu.SMEM((peers,), I32),
            pltpu.SemaphoreType.DMA((2 * entries,)),
        ],
        compiler_params=params(),
        cost_estimate=cost(1024, 1024 * 1024),
        name="routes",
    )
    held, slot_of, header = route(*tables, remap_weights)
    tables, held, header, slot_of = lax.optimization_barrier((tables, held, header, slot_of))
    near_pieces = (before, lead, last, after, across)
    far_pieces = (leads, lasts, prior, following)
    far = SURF * far_group
    close = SURF * near_group
    body = (count, far_rows, width)
    mine, back, mine_top, back_top = run_step(
        size, ring, tables, far_pieces, w, k_far, far_at,
        [body, body, (count, far, width), (count, far, width)],
        [((i // count, i % count, far_rows), (2 + i // count, i % count, far)) for i in range(2 * count)],
    )
    other = partner(back, "tile", fold_bit)
    near, near_top = run_step(
        size, 0, tables, near_pieces, w, k_near, near_at,
        [(count, near_rows, width), (count, close, width)],
        [((0, i, near_rows), (1, i, close)) for i in range(count)],
    )

    surface = SURF * fields
    groups = CAP * (close + 2 * far) // 8 + HEAD // 8
    payload_call = pl.pallas_call(
        functools.partial(partial_kernel, size),
        out_shape=shape_of((peers, groups, 8, width)),
        in_specs=[spec(SMEM)] * 3 + [spec(VMEM)] * 5,
        out_specs=spec(VMEM),
        compiler_params=params(),
        cost_estimate=cost(2 * entries * surface * width * width, 2 * 1024 * 1024),
        name="partials",
    )
    payload = payload_call(*tables[1:], slot_of, header, held, near_top, mine_top, back_top)
    payload = partner(payload, "comp", 0)
    received = lax.all_to_all(payload, "tile", split_axis=0, concat_axis=0, tiled=True)

    whole = pl.pallas_call(
        functools.partial(merge_kernel, fields, near_group, far_group, ring),
        out_shape=shape_of(plain.shape),
        in_specs=[spec(SMEM)] + [spec(VMEM)] * 3,
        out_specs=spec(VMEM),
        compiler_params=params(),
        cost_estimate=cost(2 * count * near_rows * levels * fields * width, 2 * 1024 * 1024),
        name="merge",
    )(ids, near, mine, other)
    final = pl.pallas_call(
        functools.partial(couple_kernel, fields, near_group, far_group),
        out_shape=shape_of(whole.shape),
        in_specs=[spec(SMEM), spec(HBM)] + [spec(VMEM)] * 4,
        out_specs=spec(HBM),
        input_output_aliases={1: 0},
        scratch_shapes=[
            pltpu.VMEM((count + 1, surface, width), F32),
            pltpu.VMEM((count, surface, width), BF16),
            pltpu.VMEM((HEAD, width), I32),
            pltpu.SMEM((HEAD, width), I32),
            pltpu.SemaphoreType.DMA,
        ],
        compiler_params=params(),
        cost_estimate=cost(1024, 1024 * 1024),
        name="couple",
    )(ids, whole, received, near_top, mine_top, other)
    return final.reshape(count, levels, fields, width).transpose(0, 2, 1, 3)[None]


def solution(mesh):
    return jax.shard_map(
        on_device,
        mesh=mesh,
        in_specs=(
            P("comp", "tile", None, None, None),
            P("comp", None, None, None),
            P("comp", None, None),
            P(),
            P("comp", "tile", None),
            P("comp", "tile", None),
            P("comp", "tile"),
            P("comp", "tile"),
            P("comp", "tile"),
            P("comp", "tile", None),
        ),
        out_specs=P("comp", "tile", None, None, None),
        check_vma=False,
    )
```

```python
import functools

import jax
import jax.numpy as jnp
from jax import lax
from jax.experimental import pallas as pl
from jax.experimental.pallas import tpu as pltpu
from jax.sharding import PartitionSpec as P


SURF = 8
HALO = 8
STEPS = 2
CAP = 2
HEAD = 8

VMEM = pltpu.MemorySpace.VMEM
SMEM = pltpu.MemorySpace.SMEM
HBM = pltpu.MemorySpace.HBM
BF16 = jnp.bfloat16
F32 = jnp.float32
I32 = jnp.int32


def spec(space):
    return pl.BlockSpec(memory_space=space)


def shape_of(shape, dtype=BF16):
    return jax.ShapeDtypeStruct(shape, dtype)


def params():
    return pltpu.CompilerParams(vmem_limit_bytes=16 * 1024 * 1024)


def cost(flops, moved):
    return pl.CostEstimate(flops=flops, bytes_accessed=moved, transcendentals=0)


def select_matrix(rows, wide, fields, group, first, inverse):
    shape = (wide, rows) if inverse else (rows, wide)
    mine = lax.broadcasted_iota(I32, shape, 1 if inverse else 0)
    other = lax.broadcasted_iota(I32, shape, 0 if inverse else 1)
    source = (mine // group) * fields + first + mine % group
    return jnp.where(source == other, 1.0, 0.0).astype(BF16)


def expand_kernel(group, v, k_hi, k_lo):
    rows, levels = k_hi.shape[0], v.shape[0]
    shape = (rows, levels)
    level = lax.broadcasted_iota(I32, shape, 0) // group
    spread = jnp.where(level == lax.broadcasted_iota(I32, shape, 1), 1.0, 0.0).astype(BF16)
    square = (rows, rows)
    same = (
        lax.broadcasted_iota(I32, square, 0) % group == lax.broadcasted_iota(I32, square, 1) % group
    )
    value = v[...]
    high = value.astype(BF16)
    low = (value - high.astype(F32)).astype(BF16)
    for part, out in ((high, k_hi), (low, k_lo)):
        tall = jnp.dot(spread, part, preferred_element_type=F32).astype(BF16)
        full = lax.dot_general(tall, spread, (((1,), (1,)), ((), ())), preferred_element_type=F32)
        out[...] = jnp.where(same, full, 0.0).astype(BF16)


def load_kernel(ids, w, remap, w_out, remap_out, sems):
    copies = [
        pltpu.make_async_copy(w, w_out, sems.at[0]),
        pltpu.make_async_copy(remap.at[1 - ids[1]], remap_out, sems.at[1]),
    ]
    for c in copies:
        c.start()
    for c in copies:
        c.wait()


def table_kernel(*refs):
    lists, (table, sent, taken) = refs[:6], refs[6:]
    for p in range(taken.shape[0]):
        taken[p] = 0
    at = 0
    for n, src in enumerate(lists):
        for i in range(src.shape[0]):
            for j in range(src.shape[1]):
                value = src[i, j]
                if n == 4:
                    rank = taken[value]
                    taken[value] = rank + 1
                    value = value * CAP + rank
                table[at] = value
                sent[at] = value
                at += 1


def groups_of(group, near, ring, ids):
    odd = ids[0] % 2
    low = jnp.where(ids[0] < ring, 1, 0)
    return (1 - odd) * group, odd * group, near + low * group, near + (1 - low) * group


def split_kernel(fields, group, ring, ids, x, *outs):
    rows, width = outs[0].shape[1:]
    firsts = groups_of(group, 2 * group, ring, ids)
    picks = [select_matrix(rows, x.shape[1], fields, group, f, False) for f in firsts]
    pick = jnp.concatenate(picks, axis=0)
    for b in range(0, x.shape[0], 2):
        pair = jnp.concatenate([x[b], x[b + 1]], axis=1)
        got = jnp.dot(pick, pair, preferred_element_type=F32).astype(BF16)
        for j, dst in enumerate(outs):
            for i in range(2):
                dst[b + i] = got[j * rows : (j + 1) * rows, i * width : (i + 1) * width]


def edges(ids, leads, lasts, up, down):
    odd = ids[0] % 2
    up[...] = lasts[pl.ds((1 - odd) * HALO, HALO)]
    down[...] = leads[pl.ds(odd * HALO, HALO)]


def pack_kernel(ids, mine, other, leads, lasts, *ends):
    half = leads.shape[0] // 2
    for i, src in enumerate((mine, other)):
        leads[pl.ds(i * half, half)] = src[pl.ds(0, half)]
        lasts[pl.ds(i * half, half)] = src[pl.ds(half, half)]
    if ends:
        edges(ids, leads, lasts, *ends)


def pair_index(slot, x, odd, count):
    second = x + odd - 2 * x * odd
    inner = slot - HALO
    later = inner - count
    home = jnp.where(inner < HALO, x * HALO + inner, HALO + x * HALO + inner)
    after = jnp.where(second == 1, 3 * count + HALO + later, (1 - x) * HALO + later)
    beyond = jnp.where(later < HALO, after, 2 * count + x * HALO + later - HALO)
    inside = jnp.where(inner < count, home, beyond)
    before = jnp.where(second == 1, count + (1 - x) * HALO + slot, 3 * count + slot)
    return jnp.where(inner < 0, before, inside)


def far_index(slot, x, at, ring, count):
    side_before = jnp.where(at == 0, 1 - x, x)
    side_after = jnp.where(at == ring - 1, 1 - x, x)
    inner = slot - HALO
    later = inner - count
    home = jnp.where(inner < HALO, x * HALO + inner, HALO + x * HALO + inner)
    beyond = jnp.where(
        later < HALO, 3 * count + side_after * HALO + later, (1 - x) * HALO + later - HALO
    )
    inside = jnp.where(inner < count, home, beyond)
    return jnp.where(inner < 0, 2 * count + side_before * HALO + slot, inside)


def step_kernel(pieces, size, ring, own_at, writes, ids, own, mate, *refs):
    sources, (w, k_hi, k_lo) = refs[:pieces], refs[pieces : pieces + 3]
    outs, (pool, mid, hi, lo) = refs[pieces + 3 : -4], refs[-4:]
    at = 0
    for src in sources:
        n = src.shape[0]
        pool[pl.ds(at, n)] = src[...]
        at += n
    count = len(own_at)
    stride = count // 2
    width = w.shape[1]
    for b in range(count):
        total = pool[own_at[b]].astype(F32)
        x, table = b // stride, mate if b >= stride else own
        entries = range(b % stride, size, stride)
        where = [table[e] for e in entries]
        if ring:
            where = [far_index(slot, x, ids[0] % ring, ring, stride) for slot in where]
        else:
            where = [pair_index(slot, x, ids[0] % 2, stride) for slot in where]
        what = [table[size + e] for e in entries]
        for k in range(0, len(what), 2):
            lhs = jnp.concatenate([pool[where[k]], pool[where[k + 1]]], axis=1)
            rhs = jnp.concatenate([w[what[k]], w[what[k + 1]]], axis=0)
            total = total + jnp.dot(lhs, rhs, preferred_element_type=F32)
        lanes = slice(b * width, (b + 1) * width)
        mid[:, lanes] = total
        top = total.astype(BF16)
        hi[:, lanes] = top
        lo[:, lanes] = (total - top.astype(F32)).astype(BF16)
    big, small = k_hi[...], k_lo[...]
    for b in range(0, count, 2):
        lanes = slice(b * width, (b + 2) * width)
        mixed = jnp.dot(big, hi[:, lanes], preferred_element_type=F32)
        mixed = mixed + jnp.dot(big, lo[:, lanes], preferred_element_type=F32)
        mixed = mixed + jnp.dot(small, hi[:, lanes], preferred_element_type=F32)
        new = (mid[:, lanes] + jnp.tanh(mixed)).astype(BF16)
        for i in range(2):
            for out, place, rows in writes[b + i]:
                outs[out][place] = new[:rows, i * width : (i + 1) * width]
    if not ring and outs[2].shape[0] == HALO:
        edges(ids, *outs)


def run_step(size, ring, tables, pieces, w, k, own_at, outs, writes):
    _, rows, width = pieces[0].shape
    count = len(own_at)
    total = sum(p.shape[0] for p in pieces)
    return pl.pallas_call(
        functools.partial(step_kernel, len(pieces), size, ring, own_at, writes),
        out_shape=[shape_of(o) for o in outs],
        in_specs=[spec(SMEM)] * 3 + [spec(VMEM)] * len(pieces) + [spec(VMEM)] * 3,
        out_specs=[spec(VMEM)] * len(outs),
        scratch_shapes=[
            pltpu.VMEM((total, rows, width), BF16),
            pltpu.VMEM((rows, count * width), F32),
            pltpu.VMEM((rows, count * width), BF16),
            pltpu.VMEM((rows, count * width), BF16),
        ],
        compiler_params=params(),
        cost_estimate=cost(4 * 2 * count * rows * width * width, 8 * 1024 * 1024),
    )(*tables, *pieces, w, *k)


def partial_kernel(size, entries, ids, own, pair, far, weights, *rest):
    pair_mine, pair_back, far_mine, far_back, payload = rest
    thin = pair_mine.shape[1] // 8
    head = payload.shape[1] - HEAD // 8
    payload[...] = jnp.zeros(payload.shape, payload.dtype)
    shape = payload.shape[2:]
    flat = lax.broadcasted_iota(I32, shape, 0) * shape[1] + lax.broadcasted_iota(I32, shape, 1)
    flat = flat - ids[0] * 3 * CAP
    for e in range(3 * entries):
        kind = e // entries
        table, at = (own, pair, far)[kind], 2 * size + e % entries
        src, slot = table[at], table[at + 2 * entries]
        place, rank = slot // CAP, slot % CAP
        if kind == 0:
            rows, groups, base = jnp.concatenate([pair_mine[src], far_mine[src]], axis=0), 2 * thin, 0
        else:
            rows = (pair_back if kind == 1 else far_back)[src]
            groups, base = thin, CAP * thin * (1 + kind)
        value = jnp.dot(rows, weights[table[at + entries]], preferred_element_type=F32)
        value = value.reshape(groups, 8, value.shape[1]).astype(BF16)
        payload[place, pl.ds(base + rank * groups, groups)] = value
        mark = (table[at + 3 * entries] + 1).astype(F32)
        old = payload[place, head].astype(F32)
        payload[place, head] = jnp.where(flat == kind * CAP + rank, mark, old).astype(BF16)


def merge_kernel(fields, group, ring, ids, pair_mine, pair_other, far_mine, far_other, out):
    _, wide, width = out.shape
    rows = pair_mine.shape[1]
    firsts = groups_of(group, 2 * group, ring, ids)
    picks = [select_matrix(rows, wide, fields, group, f, True) for f in firsts]
    for b in range(0, out.shape[0], 2):
        got = None
        for pick, s in zip(picks, (pair_other, pair_mine, far_other, far_mine)):
            part = jnp.concatenate([s[b], s[b + 1]], axis=1)
            part = jnp.dot(pick, part, preferred_element_type=F32)
            got = part if got is None else got + part
        got = got.astype(BF16)
        out[b] = got[:, :width]
        out[b + 1] = got[:, width:]


def couple_kernel(fields, group, ids, state, received, *rest):
    pair_mine, pair_other, far_mine, far_other, out, total, top, found, targets, sem = rest
    del state
    count, rows, width = top.shape
    peers = received.shape[0]
    part = pair_mine.shape[1]
    thin = part // 8
    heads = received[:, received.shape[1] - HEAD // 8].astype(F32)
    found[...] = jnp.sum(heads, axis=0).astype(I32)
    copy = pltpu.make_async_copy(found, targets, sem)
    copy.start()
    total[...] = jnp.zeros(total.shape, F32)
    copy.wait()
    for p in range(peers):
        close = part * (p % 2)
        side = 2 * part if p < peers // 2 else 3 * part
        for i in range(3 * CAP):
            q = p * 3 * CAP + i
            t = targets[q // width, q % width]
            kind, at = i // CAP, i % CAP
            if kind == 0:
                got = received[p, 2 * thin * at : 2 * thin * (at + 1)].astype(F32)
                got = got.reshape(2 * part, width)
                total[t, close : close + part] = total[t, close : close + part] + got[:part]
                total[t, side : side + part] = total[t, side : side + part] + got[part:]
            else:
                base = CAP * thin * (1 + kind) + at * thin
                got = received[p, base : base + thin].astype(F32).reshape(part, width)
                here = close if kind == 1 else side
                total[t, here : here + part] = total[t, here : here + part] + got
    shape = (rows, rows)
    have = lax.broadcasted_iota(I32, shape, 1)
    field = have // part * group + have % part % group
    want = have % part // group * fields + field
    pick = jnp.where(want == lax.broadcasted_iota(I32, shape, 0), 1.0, 0.0).astype(BF16)
    even = ids[0] % 2 == 0
    is_low = ids[0] < peers // 2
    for g in range(count):
        base = []
        for first, mine, other in ((even, pair_mine, pair_other), (is_low, far_mine, far_other)):
            here, there = mine[g].astype(F32), other[g, :part].astype(F32)
            base += [jnp.where(first, here, there), jnp.where(first, there, here)]
        new = (jnp.concatenate(base, axis=0) + total[g + 1]).astype(BF16)
        top[g] = jnp.dot(pick, new, preferred_element_type=F32).astype(BF16)
    copy = pltpu.make_async_copy(top, out.at[:, pl.ds(0, rows)], sem)
    copy.start()
    copy.wait()


def partner(value, axis, distance):
    mask = 2**distance
    pairs = [(source, source ^ mask) for source in range(lax.axis_size(axis))]
    return lax.ppermute(value, axis, pairs)


def shift(last, lead, ring, stride):
    peers = lax.axis_size("tile")
    up = [(i, i // ring * ring + (i + stride) % ring) for i in range(peers)]
    down = [(j, i) for i, j in up]
    before = lax.ppermute(last, "tile", up)
    return before, lax.ppermute(lead, "tile", down)


def on_device(
    state,
    dyn_weights,
    vertical,
    remap_weights,
    neighbor_slots,
    neighbor_tiles,
    remap_source,
    remap_target,
    remap_tile,
    remap_dest,
):
    _, count, fields, levels, width = state.shape
    group = fields // 4
    rows = -(-levels * group // 16) * 16
    peers = lax.axis_size("tile")
    ring = peers // 2
    fold_bit = peers.bit_length() - 2
    ids = jnp.stack([lax.axis_index("tile"), lax.axis_index("comp")])
    w = dyn_weights[0]
    plain = state[0].transpose(0, 2, 1, 3).reshape(count, levels * fields, width)
    body = (count, rows, width)

    pair_sent, pair_mine, far_sent, far_mine = pl.pallas_call(
        functools.partial(split_kernel, fields, group, ring),
        out_shape=[shape_of(body)] * 4,
        in_specs=[spec(SMEM), spec(VMEM)],
        out_specs=[spec(VMEM)] * 4,
        compiler_params=params(),
        cost_estimate=cost(8 * count * rows * levels * fields * width, 2 * 1024 * 1024),
        name="split",
    )(ids, plain)
    far_other = partner(far_sent, "tile", fold_bit)
    pair_other = partner(pair_sent, "tile", 0)

    lists = (neighbor_slots[0].T, neighbor_tiles[0].T, remap_source, remap_tile, remap_dest[:, :, 0], remap_target)
    size, entries = lists[0].size, remap_source.shape[1]
    own_table, sent_table = pl.pallas_call(
        table_kernel,
        out_shape=[shape_of((2 * size + 4 * entries,), I32)] * 2,
        in_specs=[spec(SMEM)] * len(lists),
        out_specs=[spec(SMEM)] * 2,
        scratch_shapes=[pltpu.SMEM((peers,), I32)],
        name="table",
    )(*lists)
    far_table = partner(sent_table, "tile", fold_bit)
    pair_table = partner(sent_table, "tile", 0)

    def pack(mine, other, ends):
        return pl.pallas_call(
            pack_kernel,
            out_shape=[shape_of(body)] * 2 + [shape_of((HALO, rows, width))] * ends,
            in_specs=[spec(SMEM)] + [spec(VMEM)] * 2,
            out_specs=[spec(VMEM)] * (2 + ends),
            compiler_params=params(),
            cost_estimate=cost(1024, 1024 * 1024),
            name="pack",
        )(ids, mine, other)

    pair_leads, pair_lasts, up, down = pack(pair_mine, pair_other, 2)
    expand = pl.pallas_call(
        functools.partial(expand_kernel, group),
        out_shape=[shape_of((rows, rows))] * 2,
        in_specs=[spec(VMEM)],
        out_specs=[spec(VMEM)] * 2,
        compiler_params=params(),
        cost_estimate=cost(8 * rows * rows * levels, 1024 * 1024),
        name="expand",
    )
    load = pl.pallas_call(
        load_kernel,
        out_shape=[shape_of(w.shape), shape_of(remap_weights.shape[1:])],
        in_specs=[spec(SMEM)] + [spec(HBM)] * 2,
        out_specs=[spec(VMEM)] * 2,
        scratch_shapes=[pltpu.SemaphoreType.DMA((2,))],
        compiler_params=params(),
        cost_estimate=cost(1024, 8 * 1024 * 1024),
        name="load",
    )
    k = expand(vertical[0])
    w, remap = load(ids, w, remap_weights)
    far_other, k, w, remap = lax.optimization_barrier((far_other, k, w, remap))
    tables = (own_table, pair_table, far_table)
    leads, lasts = pack(far_mine, far_other, 0)

    tail = 2 * HALO
    places = tuple(
        x * HALO + i if i < HALO else tail + x * (count - HALO) + i - HALO
        for x in range(2)
        for i in range(count)
    )
    onward = [((i % count >= HALO, p if i % count < HALO else p - tail, rows),) for i, p in enumerate(places)]
    part = SURF * group
    finish = [((i // count, i % count, rows), (2 + i // count, i % count, part)) for i in range(2 * count)]
    ended = [body, body, (count, part, width), (count, part, width)]
    edge = (HALO, rows, width)
    for step in range(STEPS):
        across = partner(pair_leads, "tile", fold_bit)
        before, after = shift(up, down, peers, 2)
        prior, following = shift(lasts, leads, ring, 1)
        pair_pieces = (pair_leads, pair_lasts, across, before, after)
        far_pieces = (leads, lasts, prior, following)
        pair_ids, far_ids = (ids, tables[0], tables[1]), (ids, tables[0], tables[2])
        if step < STEPS - 1:
            pair_leads, pair_lasts, up, down = run_step(
                size, 0, pair_ids, pair_pieces, w, k, places, [body, body, edge, edge], onward
            )
            leads, lasts = run_step(size, ring, far_ids, far_pieces, w, k, places, [body, body], onward)
    pair_mine, pair_back, pair_top, pair_back_top = run_step(
        size, 0, (ids, tables[0], tables[1]), pair_pieces, w, k, places, ended, finish
    )
    far_mine, far_back, far_top, far_back_top = run_step(
        size, ring, (ids, tables[0], tables[2]), far_pieces, w, k, places, ended, finish
    )
    pair_other = partner(pair_back, "tile", 0)
    far_other = partner(far_back, "tile", fold_bit)

    surface = SURF * fields
    payload_call = pl.pallas_call(
        functools.partial(partial_kernel, size, entries),
        out_shape=shape_of((peers, CAP * surface // 8 + HEAD // 8, 8, width)),
        in_specs=[spec(SMEM)] * 4 + [spec(VMEM)] * 5,
        out_specs=spec(VMEM),
        compiler_params=params(),
        cost_estimate=cost(2 * entries * surface * width * width, 2 * 1024 * 1024),
        name="partials",
    )
    payload = payload_call(ids, *tables, remap, pair_top, pair_back_top, far_top, far_back_top)
    payload = partner(payload, "comp", 0)
    received = lax.all_to_all(payload, "tile", split_axis=0, concat_axis=0, tiled=True)

    whole = pl.pallas_call(
        functools.partial(merge_kernel, fields, group, ring),
        out_shape=shape_of(plain.shape),
        in_specs=[spec(SMEM)] + [spec(VMEM)] * 4,
        out_specs=spec(VMEM),
        compiler_params=params(),
        cost_estimate=cost(8 * count * rows * levels * fields * width, 2 * 1024 * 1024),
        name="merge",
    )(ids, pair_mine, pair_other, far_mine, far_other)
    final = pl.pallas_call(
        functools.partial(couple_kernel, fields, group),
        out_shape=shape_of(whole.shape),
        in_specs=[spec(SMEM), spec(HBM)] + [spec(VMEM)] * 5,
        out_specs=spec(HBM),
        input_output_aliases={1: 0},
        scratch_shapes=[
            pltpu.VMEM((count + 1, surface, width), F32),
            pltpu.VMEM((count, surface, width), BF16),
            pltpu.VMEM((HEAD, width), I32),
            pltpu.SMEM((HEAD, width), I32),
            pltpu.SemaphoreType.DMA,
        ],
        compiler_params=params(),
        cost_estimate=cost(1024, 1024 * 1024),
        name="couple",
    )(ids, whole, received, pair_top, pair_other, far_top, far_other)
    return final.reshape(count, levels, fields, width).transpose(0, 2, 1, 3)[None]


def solution(mesh):
    return jax.shard_map(
        on_device,
        mesh=mesh,
        in_specs=(
            P("comp", "tile", None, None, None),
            P("comp", None, None, None),
            P("comp", None, None),
            P(),
            P("comp", "tile", None),
            P("comp", "tile", None),
            P("comp", "tile"),
            P("comp", "tile"),
            P("comp", "tile"),
            P("comp", "tile", None),
        ),
        out_specs=P("comp", "tile", None, None, None),
        check_vma=False,
    )
```

```python
import functools

import jax
import jax.numpy as jnp
from jax import lax
from jax.experimental import pallas as pl
from jax.experimental.pallas import tpu as pltpu
from jax.sharding import PartitionSpec as P


SURF = 8
HALO = 8
STEPS = 2
CAP = 2
HEAD = 8

VMEM = pltpu.MemorySpace.VMEM
SMEM = pltpu.MemorySpace.SMEM
HBM = pltpu.MemorySpace.HBM
BF16 = jnp.bfloat16
F32 = jnp.float32
I32 = jnp.int32


def spec(space):
    return pl.BlockSpec(memory_space=space)


def shape_of(shape, dtype=BF16):
    return jax.ShapeDtypeStruct(shape, dtype)


def params():
    return pltpu.CompilerParams(vmem_limit_bytes=16 * 1024 * 1024)


def cost(flops, moved):
    return pl.CostEstimate(flops=flops, bytes_accessed=moved, transcendentals=0)


def select_matrix(rows, wide, fields, group, first, inverse):
    shape = (wide, rows) if inverse else (rows, wide)
    mine = lax.broadcasted_iota(I32, shape, 1 if inverse else 0)
    other = lax.broadcasted_iota(I32, shape, 0 if inverse else 1)
    source = (mine // group) * fields + first + mine % group
    return jnp.where(source == other, 1.0, 0.0).astype(BF16)


def expand_kernel(group, v, k):
    rows, levels = k.shape[0] // 2, v.shape[0]
    shape = (rows, levels)
    level = lax.broadcasted_iota(I32, shape, 0) // group
    spread = jnp.where(level == lax.broadcasted_iota(I32, shape, 1), 1.0, 0.0).astype(BF16)
    square = (rows, rows)
    same = (
        lax.broadcasted_iota(I32, square, 0) % group == lax.broadcasted_iota(I32, square, 1) % group
    )
    value = v[...]
    high = value.astype(BF16)
    low = (value - high.astype(F32)).astype(BF16)
    k[...] = jnp.zeros(k.shape, k.dtype)
    for part, at in ((high, 0), (low, rows)):
        tall = jnp.dot(spread, part, preferred_element_type=F32).astype(BF16)
        full = lax.dot_general(tall, spread, (((1,), (1,)), ((), ())), preferred_element_type=F32)
        full = jnp.where(same, full, 0.0).astype(BF16)
        k[at : at + rows, :rows] = full
        if at == 0:
            k[:rows, rows:] = full


def load_kernel(w, w_out, sem):
    copy = pltpu.make_async_copy(w, w_out, sem)
    copy.start()
    copy.wait()


def load_half_kernel(ids, remap, out, sem):
    copy = pltpu.make_async_copy(remap.at[1 - ids[1]], out, sem)
    copy.start()
    copy.wait()


def table_kernel(*refs):
    lists, (table, sent, taken) = refs[:6], refs[6:]
    for p in range(taken.shape[0]):
        taken[p] = 0
    at = 0
    for n, src in enumerate(lists):
        for i in range(src.shape[0]):
            for j in range(src.shape[1]):
                value = src[i, j]
                if n == 4:
                    rank = taken[value]
                    taken[value] = rank + 1
                    value = value * CAP + rank
                table[at] = value
                sent[at] = value
                at += 1


def groups_of(group, near, ring, ids):
    odd = ids[0] % 2
    low = jnp.where(ids[0] < ring, 1, 0)
    return (1 - odd) * group, odd * group, near + low * group, near + (1 - low) * group


def split_kernel(fields, group, ring, ids, x, *outs):
    rows, width = outs[0].shape[1:]
    firsts = groups_of(group, 2 * group, ring, ids)
    picks = [select_matrix(rows, x.shape[1], fields, group, f, False) for f in firsts]
    pick = jnp.concatenate(picks, axis=0)
    for b in range(0, x.shape[0], 2):
        pair = jnp.concatenate([x[b], x[b + 1]], axis=1)
        got = jnp.dot(pick, pair, preferred_element_type=F32).astype(BF16)
        for j, dst in enumerate(outs):
            for i in range(2):
                dst[b + i] = got[j * rows : (j + 1) * rows, i * width : (i + 1) * width]


def edges(ids, leads, lasts, up, down):
    odd = ids[0] % 2
    up[...] = lasts[pl.ds((1 - odd) * HALO, HALO)]
    down[...] = leads[pl.ds(odd * HALO, HALO)]


def pack_kernel(ids, mine, other, leads, lasts, *ends):
    half = leads.shape[0] // 2
    for i, src in enumerate((mine, other)):
        leads[pl.ds(i * half, half)] = src[pl.ds(0, half)]
        lasts[pl.ds(i * half, half)] = src[pl.ds(half, half)]
    if ends:
        edges(ids, leads, lasts, *ends)


def pair_index(slot, x, odd, count):
    second = x + odd - 2 * x * odd
    inner = slot - HALO
    later = inner - count
    home = jnp.where(inner < HALO, x * HALO + inner, HALO + x * HALO + inner)
    after = jnp.where(second == 1, 3 * count + HALO + later, (1 - x) * HALO + later)
    beyond = jnp.where(later < HALO, after, 2 * count + x * HALO + later - HALO)
    inside = jnp.where(inner < count, home, beyond)
    before = jnp.where(second == 1, count + (1 - x) * HALO + slot, 3 * count + slot)
    return jnp.where(inner < 0, before, inside)


def far_index(slot, x, at, ring, count):
    side_before = jnp.where(at == 0, 1 - x, x)
    side_after = jnp.where(at == ring - 1, 1 - x, x)
    inner = slot - HALO
    later = inner - count
    home = jnp.where(inner < HALO, x * HALO + inner, HALO + x * HALO + inner)
    beyond = jnp.where(
        later < HALO, 3 * count + side_after * HALO + later, (1 - x) * HALO + later - HALO
    )
    inside = jnp.where(inner < count, home, beyond)
    return jnp.where(inner < 0, 2 * count + side_before * HALO + slot, inside)


def step_kernel(pieces, size, ring, own_at, writes, ids, own, mate, *refs):
    sources, (w, k) = refs[:pieces], refs[pieces : pieces + 2]
    outs, (pool, mid, halves) = refs[pieces + 2 : -3], refs[-3:]
    at = 0
    for src in sources:
        n = src.shape[0]
        pool[pl.ds(at, n)] = src[...]
        at += n
    count = len(own_at)
    stride = count // 2
    width, height = w.shape[1], mid.shape[0]
    for b in range(count):
        total = pool[own_at[b]].astype(F32)
        x, table = b // stride, mate if b >= stride else own
        entries = range(b % stride, size, stride)
        where = [table[e] for e in entries]
        if ring:
            where = [far_index(slot, x, ids[0] % ring, ring, stride) for slot in where]
        else:
            where = [pair_index(slot, x, ids[0] % 2, stride) for slot in where]
        what = [table[size + e] for e in entries]
        for e in range(0, len(what), 2):
            lhs = jnp.concatenate([pool[where[e]], pool[where[e + 1]]], axis=1)
            rhs = jnp.concatenate([w[what[e]], w[what[e + 1]]], axis=0)
            total = total + jnp.dot(lhs, rhs, preferred_element_type=F32)
        lanes = slice(b * width, (b + 1) * width)
        mid[:, lanes] = total
        top = total.astype(BF16)
        halves[:height, lanes] = top
        halves[height:, lanes] = (total - top.astype(F32)).astype(BF16)
    matrix = k[...]
    for b in range(0, count, 2):
        lanes = slice(b * width, (b + 2) * width)
        mixed = jnp.dot(matrix, halves[:, lanes], preferred_element_type=F32)
        mixed = mixed[:height] + mixed[height:]
        new = (mid[:, lanes] + jnp.tanh(mixed)).astype(BF16)
        for i in range(2):
            for out, place, rows in writes[b + i]:
                outs[out][place] = new[:rows, i * width : (i + 1) * width]
    if not ring and outs[2].shape[0] == HALO:
        edges(ids, *outs)


def run_step(size, ring, tables, pieces, w, k, own_at, outs, writes):
    _, rows, width = pieces[0].shape
    count = len(own_at)
    total = sum(p.shape[0] for p in pieces)
    return pl.pallas_call(
        functools.partial(step_kernel, len(pieces), size, ring, own_at, writes),
        out_shape=[shape_of(o) for o in outs],
        in_specs=[spec(SMEM)] * 3 + [spec(VMEM)] * len(pieces) + [spec(VMEM)] * 2,
        out_specs=[spec(VMEM)] * len(outs),
        scratch_shapes=[
            pltpu.VMEM((total, rows, width), BF16),
            pltpu.VMEM((rows, count * width), F32),
            pltpu.VMEM((2 * rows, count * width), BF16),
        ],
        compiler_params=params(),
        cost_estimate=cost(4 * 2 * count * rows * width * width, 8 * 1024 * 1024),
    )(*tables, *pieces, w, k)


def partial_kernel(size, entries, ids, own, pair, far, weights, *rest):
    pair_mine, pair_back, far_mine, far_back, payload = rest
    thin = pair_mine.shape[1] // 8
    head = payload.shape[1] - HEAD // 8
    payload[...] = jnp.zeros(payload.shape, payload.dtype)
    shape = payload.shape[2:]
    flat = lax.broadcasted_iota(I32, shape, 0) * shape[1] + lax.broadcasted_iota(I32, shape, 1)
    flat = flat - ids[0] * 3 * CAP
    for e in range(3 * entries):
        kind = e // entries
        table, at = (own, pair, far)[kind], 2 * size + e % entries
        src, slot = table[at], table[at + 2 * entries]
        place, rank = slot // CAP, slot % CAP
        if kind == 0:
            rows, groups, base = jnp.concatenate([pair_mine[src], far_mine[src]], axis=0), 2 * thin, 0
        else:
            rows = (pair_back if kind == 1 else far_back)[src]
            groups, base = thin, CAP * thin * (1 + kind)
        value = jnp.dot(rows, weights[table[at + entries]], preferred_element_type=F32)
        value = value.reshape(groups, 8, value.shape[1]).astype(BF16)
        payload[place, pl.ds(base + rank * groups, groups)] = value
        mark = (table[at + 3 * entries] + 1).astype(F32)
        old = payload[place, head].astype(F32)
        payload[place, head] = jnp.where(flat == kind * CAP + rank, mark, old).astype(BF16)


def merge_kernel(fields, group, ring, ids, pair_mine, pair_other, far_mine, far_other, out):
    _, wide, width = out.shape
    rows = pair_mine.shape[1]
    firsts = groups_of(group, 2 * group, ring, ids)
    picks = [select_matrix(rows, wide, fields, group, f, True) for f in firsts]
    for b in range(0, out.shape[0], 2):
        got = None
        for pick, s in zip(picks, (pair_other, pair_mine, far_other, far_mine)):
            part = jnp.concatenate([s[b], s[b + 1]], axis=1)
            part = jnp.dot(pick, part, preferred_element_type=F32)
            got = part if got is None else got + part
        got = got.astype(BF16)
        out[b] = got[:, :width]
        out[b + 1] = got[:, width:]


def couple_kernel(fields, group, ids, state, received, *rest):
    pair_mine, pair_other, far_mine, far_other, out, *sums, top, found, targets, sem = rest
    del state
    count, rows, width = top.shape
    peers = received.shape[0]
    part = pair_mine.shape[1]
    thin = part // 8
    heads = received[:, received.shape[1] - HEAD // 8].astype(F32)
    found[...] = jnp.sum(heads, axis=0).astype(I32)
    copy = pltpu.make_async_copy(found, targets, sem)
    copy.start()
    for total in sums:
        total[...] = jnp.zeros(total.shape, F32)
    copy.wait()
    for p in range(peers):
        close, side = sums[p % 2], sums[2 if p < peers // 2 else 3]
        for i in range(3 * CAP):
            q = p * 3 * CAP + i
            t = targets[q // width, q % width]
            kind, at = i // CAP, i % CAP
            if kind == 0:
                got = received[p, 2 * thin * at : 2 * thin * (at + 1)].astype(F32)
                got = got.reshape(2 * part, width)
                close[t] = close[t] + got[:part]
                side[t] = side[t] + got[part:]
            else:
                base = CAP * thin * (1 + kind) + at * thin
                got = received[p, base : base + thin].astype(F32).reshape(part, width)
                here = close if kind == 1 else side
                here[t] = here[t] + got
    shape = (rows, rows)
    have = lax.broadcasted_iota(I32, shape, 1)
    field = have // part * group + have % part % group
    want = have % part // group * fields + field
    pick = jnp.where(want == lax.broadcasted_iota(I32, shape, 0), 1.0, 0.0).astype(BF16)
    even = ids[0] % 2 == 0
    is_low = ids[0] < peers // 2
    for g in range(count):
        base = []
        for first, mine, other in ((even, pair_mine, pair_other), (is_low, far_mine, far_other)):
            here, there = mine[g].astype(F32), other[g, :part].astype(F32)
            base += [jnp.where(first, here, there), jnp.where(first, there, here)]
        new = [a + total[g + 1] for a, total in zip(base, sums)]
        new = jnp.concatenate(new, axis=0).astype(BF16)
        top[g] = jnp.dot(pick, new, preferred_element_type=F32).astype(BF16)
    copy = pltpu.make_async_copy(top, out.at[:, pl.ds(0, rows)], sem)
    copy.start()
    copy.wait()


def partner(value, axis, distance):
    mask = 2**distance
    pairs = [(source, source ^ mask) for source in range(lax.axis_size(axis))]
    return lax.ppermute(value, axis, pairs)


def shift(last, lead, ring, stride):
    peers = lax.axis_size("tile")
    up = [(i, i // ring * ring + (i + stride) % ring) for i in range(peers)]
    down = [(j, i) for i, j in up]
    before = lax.ppermute(last, "tile", up)
    return before, lax.ppermute(lead, "tile", down)


def on_device(
    state,
    dyn_weights,
    vertical,
    remap_weights,
    neighbor_slots,
    neighbor_tiles,
    remap_source,
    remap_target,
    remap_tile,
    remap_dest,
):
    _, count, fields, levels, width = state.shape
    group = fields // 4
    rows = -(-levels * group // 16) * 16
    peers = lax.axis_size("tile")
    ring = peers // 2
    fold_bit = peers.bit_length() - 2
    ids = jnp.stack([lax.axis_index("tile"), lax.axis_index("comp")])
    w = dyn_weights[0]
    plain = state[0].transpose(0, 2, 1, 3).reshape(count, levels * fields, width)
    body = (count, rows, width)

    pair_sent, pair_mine, far_sent, far_mine = pl.pallas_call(
        functools.partial(split_kernel, fields, group, ring),
        out_shape=[shape_of(body)] * 4,
        in_specs=[spec(SMEM), spec(VMEM)],
        out_specs=[spec(VMEM)] * 4,
        compiler_params=params(),
        cost_estimate=cost(8 * count * rows * levels * fields * width, 2 * 1024 * 1024),
        name="split",
    )(ids, plain)
    far_other = partner(far_sent, "tile", fold_bit)
    pair_other = partner(pair_sent, "tile", 0)

    lists = (neighbor_slots[0].T, neighbor_tiles[0].T, remap_source, remap_tile, remap_dest[:, :, 0], remap_target)
    size, entries = lists[0].size, remap_source.shape[1]
    own_table, sent_table = pl.pallas_call(
        table_kernel,
        out_shape=[shape_of((2 * size + 4 * entries,), I32)] * 2,
        in_specs=[spec(SMEM)] * len(lists),
        out_specs=[spec(SMEM)] * 2,
        scratch_shapes=[pltpu.SMEM((peers,), I32)],
        name="table",
    )(*lists)
    far_table = partner(sent_table, "tile", fold_bit)
    pair_table = partner(sent_table, "tile", 0)

    def pack(mine, other, ends):
        return pl.pallas_call(
            pack_kernel,
            out_shape=[shape_of(body)] * 2 + [shape_of((HALO, rows, width))] * ends,
            in_specs=[spec(SMEM)] + [spec(VMEM)] * 2,
            out_specs=[spec(VMEM)] * (2 + ends),
            compiler_params=params(),
            cost_estimate=cost(1024, 1024 * 1024),
            name="pack",
        )(ids, mine, other)

    expand = pl.pallas_call(
        functools.partial(expand_kernel, group),
        out_shape=shape_of((2 * rows, 2 * rows)),
        in_specs=[spec(VMEM)],
        out_specs=spec(VMEM),
        compiler_params=params(),
        cost_estimate=cost(8 * rows * rows * levels, 1024 * 1024),
        name="expand",
    )
    load = pl.pallas_call(
        load_kernel,
        out_shape=shape_of(w.shape),
        in_specs=[spec(HBM)],
        out_specs=spec(VMEM),
        scratch_shapes=[pltpu.SemaphoreType.DMA],
        compiler_params=params(),
        cost_estimate=cost(1024, 4 * 1024 * 1024),
        name="load",
    )
    k = expand(vertical[0])
    w = load(w)
    pair_other, k, w = lax.optimization_barrier((pair_other, k, w))
    tables = (own_table, pair_table, far_table)

    pair_leads, pair_lasts, up, down = pack(pair_mine, pair_other, 2)
    leads, lasts = pack(far_mine, far_other, 0)

    tail = 2 * HALO
    places = tuple(
        x * HALO + i if i < HALO else tail + x * (count - HALO) + i - HALO
        for x in range(2)
        for i in range(count)
    )
    onward = [((i % count >= HALO, p if i % count < HALO else p - tail, rows),) for i, p in enumerate(places)]
    part = SURF * group
    finish = [((i // count, i % count, rows), (2 + i // count, i % count, part)) for i in range(2 * count)]
    ended = [body, body, (count, part, width), (count, part, width)]
    edge = (HALO, rows, width)
    for step in range(STEPS):
        across = partner(pair_leads, "tile", fold_bit)
        before, after = shift(up, down, peers, 2)
        prior, following = shift(lasts, leads, ring, 1)
        pair_pieces = (pair_leads, pair_lasts, across, before, after)
        far_pieces = (leads, lasts, prior, following)
        pair_ids, far_ids = (ids, tables[0], tables[1]), (ids, tables[0], tables[2])
        if step < STEPS - 1:
            pair_leads, pair_lasts, up, down = run_step(
                size, 0, pair_ids, pair_pieces, w, k, places, [body, body, edge, edge], onward
            )
            leads, lasts = run_step(size, ring, far_ids, far_pieces, w, k, places, [body, body], onward)
    load_half = pl.pallas_call(
        load_half_kernel,
        out_shape=shape_of(remap_weights.shape[1:]),
        in_specs=[spec(SMEM), spec(HBM)],
        out_specs=spec(VMEM),
        scratch_shapes=[pltpu.SemaphoreType.DMA],
        compiler_params=params(),
        cost_estimate=cost(1024, 4 * 1024 * 1024),
        name="load",
    )
    remap = load_half(ids, remap_weights)
    tables, remap = lax.optimization_barrier((tables, remap))
    pair_mine, pair_back, pair_top, pair_back_top = run_step(
        size, 0, (ids, tables[0], tables[1]), pair_pieces, w, k, places, ended, finish
    )
    far_mine, far_back, far_top, far_back_top = run_step(
        size, ring, (ids, tables[0], tables[2]), far_pieces, w, k, places, ended, finish
    )
    pair_other = partner(pair_back, "tile", 0)
    far_other = partner(far_back, "tile", fold_bit)

    surface = SURF * fields
    payload_call = pl.pallas_call(
        functools.partial(partial_kernel, size, entries),
        out_shape=shape_of((peers, CAP * surface // 8 + HEAD // 8, 8, width)),
        in_specs=[spec(SMEM)] * 4 + [spec(VMEM)] * 5,
        out_specs=spec(VMEM),
        compiler_params=params(),
        cost_estimate=cost(2 * entries * surface * width * width, 2 * 1024 * 1024),
        name="partials",
    )
    payload = payload_call(ids, *tables, remap, pair_top, pair_back_top, far_top, far_back_top)
    payload = partner(payload, "comp", 0)
    received = lax.all_to_all(payload, "tile", split_axis=0, concat_axis=0, tiled=True)

    whole = pl.pallas_call(
        functools.partial(merge_kernel, fields, group, ring),
        out_shape=shape_of(plain.shape),
        in_specs=[spec(SMEM)] + [spec(VMEM)] * 4,
        out_specs=spec(VMEM),
        compiler_params=params(),
        cost_estimate=cost(8 * count * rows * levels * fields * width, 2 * 1024 * 1024),
        name="merge",
    )(ids, pair_mine, pair_other, far_mine, far_other)
    final = pl.pallas_call(
        functools.partial(couple_kernel, fields, group),
        out_shape=shape_of(whole.shape),
        in_specs=[spec(SMEM), spec(HBM)] + [spec(VMEM)] * 5,
        out_specs=spec(HBM),
        input_output_aliases={1: 0},
        scratch_shapes=[
            *([pltpu.VMEM((count + 1, part, width), F32)] * 4),
            pltpu.VMEM((count, surface, width), BF16),
            pltpu.VMEM((HEAD, width), I32),
            pltpu.SMEM((HEAD, width), I32),
            pltpu.SemaphoreType.DMA,
        ],
        compiler_params=params(),
        cost_estimate=cost(1024, 1024 * 1024),
        name="couple",
    )(ids, whole, received, pair_top, pair_other, far_top, far_other)
    return final.reshape(count, levels, fields, width).transpose(0, 2, 1, 3)[None]


def solution(mesh):
    return jax.shard_map(
        on_device,
        mesh=mesh,
        in_specs=(
            P("comp", "tile", None, None, None),
            P("comp", None, None, None),
            P("comp", None, None),
            P(),
            P("comp", "tile", None),
            P("comp", "tile", None),
            P("comp", "tile"),
            P("comp", "tile"),
            P("comp", "tile"),
            P("comp", "tile", None),
        ),
        out_specs=P("comp", "tile", None, None, None),
        check_vma=False,
    )
```
